32 devices in a mesh: groups: 1, section: 2 (over x), axial: 16 (over z, y, core).
Axes of the slice: x: 2, y: 2, z: 4, core: 2. Of those that a mesh axis runs over, the one named last changes fastest.
Arguments:
- pair_in: bfloat16 [4, 128, 128, 128], P('groups', 'axial'), may hold values from -6 to 6
- crop_mask: int32 [4, 128], P('groups'), may hold values 0 or 1
- proj_weights: bfloat16 [2, 5, 128, 128], P('section'), may hold values from -0.5 to 0.5
- out_weights: bfloat16 [2, 128, 128], P('section'), may hold values from -0.5 to 0.5
- up_weights: bfloat16 [2, 128, 512], P('section'), may hold values from -0.5 to 0.5
- down_weights: bfloat16 [2, 512, 128], P('section'), may hold values from -0.25 to 0.25
- norm_gains: bfloat16 [2, 3, 128], P('section'), may hold values from 0.099609375 to 1.8984375
Outputs:
- pair_out: bfloat16 [4, 128, 128, 128], P(('groups', 'section'), 'axial')
The draws below stay inside these ranges and needn't reach their ends.
Inputs may be any that keep to these rules, and one draw needn't show every extreme that they name: `crop_mask`: 1 marks a residue inside the crop, 0 a padded one.
All inputs are finite; a program needn't handle non-finite values.
Results may differ from the reference program's by a relative error of at most 0.013.
Values may be sent and summed in bfloat16 or wider, within the bound.
No kernel may reach another device: no remote copies, remote signals or barrier semaphores. Data moves between devices by JAX's collectives and lax.ppermute only.
A program may use at most 64 MiB of HBM per device.

```python
import jax
import jax.numpy as jnp
from jax import lax

C = 128
MB = 4
N = 128
BLOCKS = 2
FF = 512


def touch_ends(entries, key, smallest, high):
    extent = entries.shape
    place = [jax.random.randint(jax.random.fold_in(key, axis), (), 0, extent[axis]) for axis in range(len(extent))]
    entries = entries.at[tuple(place)].set(smallest)
    longest = extent.index(max(extent))
    place[longest] = (place[longest] + 1) % extent[longest]
    return entries.at[tuple(place)].set(high)


def shard_levels(key, extent, shards, smallest, largest):
    loudness = 1.0
    for axis_at, blocks in shards:
        steps = jax.random.uniform(jax.random.fold_in(jax.random.fold_in(key, 6), axis_at), (blocks,), jnp.float32, smallest / len(shards), largest / len(shards))
        loudness = loudness * jnp.repeat(jnp.exp(steps), extent[axis_at] // blocks).reshape((-1,) + (1,) * (len(extent) - 1 - axis_at))
    return loudness


def scatter_about(stream_key, dims, scale, reach, split=(), dtype=jnp.bfloat16):
    level = shard_levels(stream_key, dims, split, -0.22, 0.18) if split else 1.0
    drawn = jax.random.normal(stream_key, dims, jnp.float32) * scale * level
    return jnp.minimum(jnp.maximum(drawn, -reach), reach).astype(dtype)


def setup_inputs(seed: int = 0, part: int = 0) -> dict:
    splits = jax.random.split(jax.random.key(seed), 8)
    part_splits = jax.random.split(jax.random.fold_in(splits[7], part), 8)
    pair_in = scatter_about(part_splits[0], (MB, N, N, C), 1.0, 6.0, ((1, 16),))
    crop_mask = touch_ends((jax.random.randint(part_splits[1], (MB, N), 0, 8) < 7).astype(jnp.int32), jax.random.fold_in(part_splits[1], 1), 0, 1)
    proj_weights = scatter_about(splits[2], (BLOCKS, 5, C, C), C ** -0.5, 0.5, ((0, 2),))
    out_weights = scatter_about(splits[3], (BLOCKS, C, C), C ** -0.5, 0.5, ((0, 2),))
    up_weights = scatter_about(splits[4], (BLOCKS, C, FF), C ** -0.5, 0.5, ((0, 2),))
    down_weights = scatter_about(splits[5], (BLOCKS, FF, C), FF ** -0.5, 0.25, ((0, 2),))
    norm_gains = jnp.clip(1.0 + 0.18 * jax.random.normal(splits[6], (BLOCKS, 3, C), jnp.float32), 0.099609375, 1.8984375).astype(jnp.bfloat16)
    return dict(pair_in=pair_in, crop_mask=crop_mask, proj_weights=proj_weights, out_weights=out_weights, up_weights=up_weights, down_weights=down_weights, norm_gains=norm_gains)


epsilon = 1e-05

def normalize(values, axis_dim):
    center = values - lax.optimization_barrier(jnp.mean(values, axis=axis_dim, keepdims=True))
    spread = lax.optimization_barrier(jnp.mean(center * center, axis=axis_dim, keepdims=True))
    return center * lax.rsqrt(spread + epsilon)

def evo_block(current, mask_all, proj_mats, out_mat, up_mat, down_mat, gain_rows):
    channels = current.shape[2]
    gain_vals = gain_rows.astype(jnp.float32)
    pair_f = current.astype(jnp.float32)
    normed = (normalize(pair_f, 2) * gain_vals[0]).astype(jnp.bfloat16)
    linear = jnp.einsum('ijd,edc->ecij', normed.astype(jnp.float32), proj_mats[:4].astype(jnp.float32))
    pair_mask = mask_all[:, None] * mask_all[None, :]
    left_edge = (jax.nn.sigmoid(linear[1]) * linear[0] * pair_mask).astype(jnp.bfloat16)
    right_edge = (jax.nn.sigmoid(linear[3]) * linear[2] * pair_mask).astype(jnp.bfloat16)
    product = jnp.einsum('cik,cjk->cij', left_edge.astype(jnp.float32), right_edge.astype(jnp.float32)).astype(jnp.bfloat16)
    tri_norm = (normalize(product.astype(jnp.float32), 0) * gain_vals[1][:, None, None]).astype(jnp.bfloat16)
    update = jnp.einsum('cij,cd->ijd', tri_norm.astype(jnp.float32), out_mat.astype(jnp.float32))
    gate_values = jax.nn.sigmoid(jnp.einsum('ijd,dc->ijc', normed.astype(jnp.float32), proj_mats[4].astype(jnp.float32)))
    pair_mid = pair_f + gate_values * update
    trans_in = (normalize(pair_mid, 2) * gain_vals[2]).astype(jnp.bfloat16).reshape(-1, channels)
    hidden = jax.nn.relu(jnp.dot(trans_in, up_mat, preferred_element_type=jnp.float32)).astype(jnp.bfloat16)
    pair_new = pair_mid + jnp.dot(hidden, down_mat, preferred_element_type=jnp.float32).reshape(pair_mid.shape)
    return pair_new.astype(jnp.bfloat16)

def reference(pair_in, crop_mask, proj_weights, out_weights, up_weights, down_weights, norm_gains):
    finished = []
    for micro_index in range(MB):
        current = pair_in[micro_index]
        mask_all = crop_mask[micro_index].astype(jnp.float32)
        for layer_index in range(BLOCKS):
            current = evo_block(current, mask_all, proj_weights[layer_index], out_weights[layer_index], up_weights[layer_index], down_weights[layer_index], norm_gains[layer_index])
        finished.append(current)
    return jnp.stack(finished)
```

```python
import jax
import jax.numpy as jnp
from jax import lax
from jax.sharding import PartitionSpec as P

epsilon = 1e-05


def normalize(values, axis_dim):
    center = values - jnp.mean(values, axis=axis_dim, keepdims=True)
    spread = jnp.mean(center * center, axis=axis_dim, keepdims=True)
    return center * lax.rsqrt(spread + epsilon)


def swap_parts(blocks, part, parts, width):
    if parts == 1:
        return blocks
    if parts == 2:
        size = parts * width
        arrived = lax.ppermute(
            jnp.where(part == 0, blocks[1], blocks[0]),
            "axial",
            [(i, (i + width) % size) for i in range(size)],
        )
        return jnp.stack(
            (jnp.where(part == 0, blocks[0], arrived), jnp.where(part == 0, arrived, blocks[1]))
        )
    groups = [[place + p * width for p in range(parts)] for place in range(width)]
    return lax.all_to_all(blocks, "axial", 0, 0, tiled=True, axis_index_groups=groups)


def per_layer(weight, section, sections):
    slots = [weight[0]]
    for shift in range(1, sections):
        slots.append(
            lax.ppermute(
                weight[0], "section", [((i + shift) % sections, i) for i in range(sections)]
            )
        )
    layers = []
    for layer in range(sections):
        chosen = slots[0]
        for shift in range(1, sections):
            chosen = jnp.where((section + shift) % sections == layer, slots[shift], chosen)
        layers.append(chosen)
    return layers


def evo_block(current, mask_rows, mask_all, parts, width, groups, proj, out_mat, up, down, gains):
    rows, columns, channels = current.shape
    per_group = channels // width
    gain_vals = gains.astype(jnp.float32)
    pair_f = current.astype(jnp.float32)
    normed = (normalize(pair_f, 2) * gain_vals[0]).astype(jnp.bfloat16)
    linear = jnp.einsum("rnd,edc->ecrn", normed, proj[:4], preferred_element_type=jnp.float32)
    pair_mask = mask_rows[:, None] * mask_all[None, :]
    left = (jax.nn.sigmoid(linear[1]) * linear[0] * pair_mask).astype(jnp.bfloat16)
    right = (jax.nn.sigmoid(linear[3]) * linear[2] * pair_mask).astype(jnp.bfloat16)
    edges = jnp.stack((left, right)).reshape(2, width, per_group, rows, columns)
    edges = lax.all_to_all(
        edges.transpose(1, 0, 2, 3, 4), "axial", 0, 0, tiled=True, axis_index_groups=groups
    )
    full_left = edges[:, 0].transpose(1, 0, 2, 3).reshape(per_group, columns, columns)
    full_right = (
        edges[:, 1]
        .reshape(width, per_group, parts, rows // parts, columns)
        .transpose(1, 2, 0, 3, 4)
        .reshape(per_group, columns, columns)
    )
    product = jnp.einsum(
        "cik,cjk->cij", full_left, full_right, preferred_element_type=jnp.float32
    ).astype(jnp.bfloat16)
    product = product.reshape(per_group, width, rows, columns).transpose(1, 0, 2, 3)
    restored = lax.all_to_all(
        product, "axial", 0, 0, tiled=True, axis_index_groups=groups
    ).reshape(channels, rows, columns)
    tri_norm = (
        normalize(restored.astype(jnp.float32), 0) * gain_vals[1][:, None, None]
    ).astype(jnp.bfloat16)
    update = jnp.einsum("crn,cd->rnd", tri_norm, out_mat, preferred_element_type=jnp.float32)
    gate_values = jax.nn.sigmoid(
        jnp.einsum("rnd,dc->rnc", normed, proj[4], preferred_element_type=jnp.float32)
    )
    pair_mid = pair_f + gate_values * update
    trans_in = (normalize(pair_mid, 2) * gain_vals[2]).astype(jnp.bfloat16).reshape(-1, channels)
    hidden = jax.nn.relu(jnp.dot(trans_in, up, preferred_element_type=jnp.float32)).astype(
        jnp.bfloat16
    )
    pair_new = pair_mid + jnp.dot(hidden, down, preferred_element_type=jnp.float32).reshape(
        pair_mid.shape
    )
    return pair_new.astype(jnp.bfloat16)


def per_device(pair_in, crop_mask, proj_weights, out_weights, up_weights, down_weights, norm_gains):
    section = lax.axis_index("section")
    sections = lax.axis_size("section")
    axial = lax.axis_size("axial")
    here = lax.axis_index("axial")
    own_count = pair_in.shape[0] // sections
    rows, columns, channels = pair_in.shape[1:]
    parts = own_count
    width = axial // parts
    part, place = here // width, here % width
    groups = [[p * width + i for i in range(width)] for p in range(parts)]
    weights = [
        per_layer(w, section, sections)
        for w in (proj_weights, out_weights, up_weights, down_weights, norm_gains)
    ]
    own_pairs = lax.dynamic_slice_in_dim(pair_in, section * own_count, own_count, 0)
    mask_all = lax.dynamic_index_in_dim(
        crop_mask, section * own_count + part, 0, keepdims=False
    ).astype(jnp.float32)
    mask_rows = lax.dynamic_slice_in_dim(
        mask_all.reshape(parts, width * rows), place * rows, rows, 1
    ).reshape(parts * rows)
    current = swap_parts(own_pairs, part, parts, width).reshape(parts * rows, columns, channels)
    for layer in range(sections):
        current = evo_block(
            current, mask_rows, mask_all, parts, width, groups, *[w[layer] for w in weights]
        )
    return swap_parts(current.reshape(parts, rows, columns, channels), part, parts, width)


def solution(mesh):
    return jax.shard_map(
        per_device,
        mesh=mesh,
        in_specs=(
            P("groups", "axial", None, None),
            P("groups", None),
            P("section", None, None, None),
            P("section", None, None),
            P("section", None, None),
            P("section", None, None),
            P("section", None, None),
        ),
        out_specs=P(("groups", "section"), "axial", None, None),
        check_vma=False,
    )
```

```python
import jax
import jax.numpy as jnp
from jax import lax
from jax.sharding import PartitionSpec as P

epsilon = 1e-05


def normalize(values, axis_dim):
    center = values - jnp.mean(values, axis=axis_dim, keepdims=True)
    spread = jnp.mean(center * center, axis=axis_dim, keepdims=True)
    return center * lax.rsqrt(spread + epsilon)


def swap_parts(blocks, part, parts, width):
    if parts == 1:
        return blocks
    if parts == 2:
        size = parts * width
        arrived = lax.ppermute(
            jnp.where(part == 0, blocks[1], blocks[0]),
            "axial",
            [(i, (i + width) % size) for i in range(size)],
        )
        return jnp.stack(
            (jnp.where(part == 0, blocks[0], arrived), jnp.where(part == 0, arrived, blocks[1]))
        )
    groups = [[place + p * width for p in range(parts)] for place in range(width)]
    return lax.all_to_all(blocks, "axial", 0, 0, tiled=True, axis_index_groups=groups)


def per_layer(weight, section, sections):
    slots = [weight[0]]
    for shift in range(1, sections):
        slots.append(
            lax.ppermute(
                weight[0], "section", [((i + shift) % sections, i) for i in range(sections)]
            )
        )
    layers = []
    for layer in range(sections):
        chosen = slots[0]
        for shift in range(1, sections):
            chosen = jnp.where((section + shift) % sections == layer, slots[shift], chosen)
        layers.append(chosen)
    return layers


def triangle(normed, mask_rows, mask_all, parts, width, groups, proj):
    rows, columns, channels = normed.shape
    per_group = channels // width
    linear = jnp.einsum("rnd,edc->ecrn", normed, proj[:4], preferred_element_type=jnp.float32)
    pair_mask = mask_rows[:, None] * mask_all[None, :]
    left = (jax.nn.sigmoid(linear[1]) * linear[0] * pair_mask).astype(jnp.bfloat16)
    right = (jax.nn.sigmoid(linear[3]) * linear[2] * pair_mask).astype(jnp.bfloat16)
    edges = jnp.stack((left, right)).reshape(2, width, per_group, rows, columns)
    edges = lax.all_to_all(
        edges.transpose(1, 0, 2, 3, 4), "axial", 0, 0, tiled=True, axis_index_groups=groups
    )
    full_left = edges[:, 0].transpose(1, 0, 2, 3).reshape(per_group, columns, columns)
    full_right = (
        edges[:, 1]
        .reshape(width, per_group, parts, rows // parts, columns)
        .transpose(1, 2, 0, 3, 4)
        .reshape(per_group, columns, columns)
    )
    return jnp.einsum(
        "cik,cjk->cij", full_left, full_right, preferred_element_type=jnp.float32
    ).astype(jnp.bfloat16)


def finish(restored, pair_f, normed, proj, out_mat, up, down, gain_vals):
    channels = pair_f.shape[2]
    tri_norm = (
        normalize(restored.astype(jnp.float32), 1) * gain_vals[1][:, None, None]
    ).astype(jnp.bfloat16)
    update = jnp.einsum("pcrn,cd->prnd", tri_norm, out_mat, preferred_element_type=jnp.float32)
    gate_values = jax.nn.sigmoid(
        jnp.einsum("rnd,dc->rnc", normed, proj[4], preferred_element_type=jnp.float32)
    )
    pair_mid = pair_f + gate_values * update.reshape(pair_f.shape)
    trans_in = (normalize(pair_mid, 2) * gain_vals[2]).astype(jnp.bfloat16).reshape(-1, channels)
    hidden = jax.nn.relu(jnp.dot(trans_in, up, preferred_element_type=jnp.float32)).astype(
        jnp.bfloat16
    )
    pair_new = pair_mid + jnp.dot(hidden, down, preferred_element_type=jnp.float32).reshape(
        pair_mid.shape
    )
    return pair_new.astype(jnp.bfloat16)


def per_device(pair_in, crop_mask, proj_weights, out_weights, up_weights, down_weights, norm_gains):
    section = lax.axis_index("section")
    sections = lax.axis_size("section")
    axial = lax.axis_size("axial")
    here = lax.axis_index("axial")
    own_count = pair_in.shape[0] // sections
    rows, columns, channels = pair_in.shape[1:]
    parts = own_count
    width = axial // parts
    per_group = channels // width
    part, place = here // width, here % width
    groups = [[p * width + i for i in range(width)] for p in range(parts)]
    weights = [
        per_layer(w, section, sections)
        for w in (proj_weights, out_weights, up_weights, down_weights, norm_gains)
    ]
    own_pairs = lax.dynamic_slice_in_dim(pair_in, section * own_count, own_count, 0)
    mask_all = lax.dynamic_index_in_dim(
        crop_mask, section * own_count + part, 0, keepdims=False
    ).astype(jnp.float32)
    mask_rows = lax.dynamic_slice_in_dim(
        mask_all.reshape(parts, width * rows), place * rows, rows, 1
    ).reshape(parts * rows)
    current = swap_parts(own_pairs, part, parts, width).reshape(parts * rows, columns, channels)
    for layer in range(sections):
        proj, out_mat, up, down, gains = [w[layer] for w in weights]
        gain_vals = gains.astype(jnp.float32)
        pair_f = current.astype(jnp.float32)
        normed = (normalize(pair_f, 2) * gain_vals[0]).astype(jnp.bfloat16)
        product = triangle(normed, mask_rows, mask_all, parts, width, groups, proj)
        product = product.reshape(per_group, width, parts, rows, columns)
        if layer < sections - 1:
            restored = lax.all_to_all(
                product.transpose(1, 0, 2, 3, 4), "axial", 0, 0, tiled=True, axis_index_groups=groups
            )
            restored = restored.reshape(channels, parts, rows, columns).transpose(1, 0, 2, 3)
        else:
            restored = lax.all_to_all(
                product.transpose(2, 1, 0, 3, 4).reshape(axial, per_group, rows, columns),
                "axial", 0, 0, tiled=True,
            ).reshape(parts, channels, rows, columns)
            current = swap_parts(
                current.reshape(parts, rows, columns, channels), part, parts, width
            ).reshape(current.shape)
            pair_f = current.astype(jnp.float32)
            normed = (normalize(pair_f, 2) * gain_vals[0]).astype(jnp.bfloat16)
        current = finish(restored, pair_f, normed, proj, out_mat, up, down, gain_vals)
    return current.reshape(parts, rows, columns, channels)


def solution(mesh):
    return jax.shard_map(
        per_device,
        mesh=mesh,
        in_specs=(
            P("groups", "axial", None, None),
            P("groups", None),
            P("section", None, None, None),
            P("section", None, None),
            P("section", None, None),
            P("section", None, None),
            P("section", None, None),
        ),
        out_specs=P(("groups", "section"), "axial", None, None),
        check_vma=False,
    )
```

```python
import functools

import jax
import jax.numpy as jnp
from jax import lax
from jax.experimental import pallas as pl
from jax.experimental.pallas import tpu as pltpu
from jax.sharding import PartitionSpec as P

epsilon = 1e-05
LANES = 128
VMEM_BYTES = 48 * 1024 * 1024


def sigmoid(x):
    return 0.5 * jnp.tanh(0.5 * x) + 0.5


def normalize(values):
    count = values.shape[0]
    center = values - jnp.sum(values, axis=0, keepdims=True) * (1.0 / count)
    spread = jnp.sum(center * center, axis=0, keepdims=True) * (1.0 / count)
    return center * lax.rsqrt(spread + epsilon)


def matmul(a, b):
    return jnp.dot(a, b, preferred_element_type=jnp.float32)


def put_row(scratch, row, rows, values):
    for tile in range(scratch.shape[0]):
        scratch[tile, pl.ds(row, values.shape[0], stride=rows), :] = values[
            :, tile * LANES : (tile + 1) * LANES
        ]


def take_row(scratch, row, rows, channels):
    tiles = [
        scratch[tile, pl.ds(row, channels, stride=rows), :] for tile in range(scratch.shape[0])
    ]
    return tiles[0] if len(tiles) == 1 else jnp.concatenate(tiles, axis=1)


def edges_of_row(pair_f, row, rows, mask, proj, gain, left_scr, right_scr):
    channels = pair_f.shape[0]
    normed = (normalize(pair_f) * gain).astype(jnp.bfloat16)
    linear = matmul(proj[...], normed)
    p0, p1, p2, p3, p4 = [linear[e * channels : (e + 1) * channels] for e in range(5)]
    put_row(left_scr, row, rows, sigmoid(p1) * p0 * mask)
    put_row(right_scr, row, rows, sigmoid(p3) * p2 * mask)
    return sigmoid(p4)


def write_edges(left_scr, right_scr, chunk, edges):
    groups, _, _, block, columns = edges.shape
    for which, scr in enumerate((left_scr, right_scr)):
        for group in range(groups):
            for tile in range(columns // LANES):
                edges[group, chunk, which, :, tile * LANES : (tile + 1) * LANES] = scr[
                    tile, pl.ds(group * block, block), :
                ].astype(jnp.bfloat16)


def first_kernel(pair, mask, proj, gains, edges, pair_t, gate, left_scr, right_scr):
    chunks, rows = pair.shape[:2]
    for chunk in range(chunks):

        def step(row, carry):
            pair_f = pair[chunk, row].astype(jnp.float32).T
            pair_t[chunk, row] = pair_f.astype(jnp.bfloat16)
            gate[chunk, row] = edges_of_row(
                pair_f, row, rows, mask[chunk, row], proj, gains[0], left_scr, right_scr
            )
            return carry

        lax.fori_loop(0, rows, step, 0)
        write_edges(left_scr, right_scr, chunk, edges)


def triangle_kernel(edges, product, wide, sums):
    groups, chunks, _, block, columns = edges.shape
    rows = columns // (groups * chunks)
    for group in range(groups):
        for chunk in range(chunks):
            for which in range(2):
                wide[which, chunk * groups + group] = edges[group, chunk, which].astype(jnp.float32)
    places = groups * chunks

    def step(c, carry):
        at = pl.ds(pl.multiple_of(c * rows, rows), rows)
        left, right = [
            jnp.concatenate([wide[which, p, at, :] for p in range(places)], axis=0).astype(
                jnp.bfloat16
            )
            for which in range(2)
        ]
        total = lax.dot_general(
            left, right, (((1,), (1,)), ((), ())), preferred_element_type=jnp.float32
        )
        for p in range(places):
            sums[p, at, :] = total[p * rows : (p + 1) * rows]
        return carry

    lax.fori_loop(0, block // rows, step, 0)
    for group in range(groups):
        for chunk in range(chunks):
            product[group, chunk] = sums[chunk * groups + group].astype(jnp.bfloat16)


def load_product(product, chunk, prod_scr):
    groups, _, block, columns = product.shape
    for group in range(groups):
        for tile in range(columns // LANES):
            prod_scr[tile, pl.ds(group * block, block), :] = product[
                group, chunk, :, tile * LANES : (tile + 1) * LANES
            ].astype(jnp.float32)


def finish_row(tri, pair_f, gate, out_t, up_t, down_t, gains):
    tri_norm = (normalize(tri) * gains[1]).astype(jnp.bfloat16)
    mid = pair_f + gate * matmul(out_t[...], tri_norm)
    trans_in = (normalize(mid) * gains[2]).astype(jnp.bfloat16)
    hidden = jnp.maximum(matmul(up_t[...], trans_in), 0.0).astype(jnp.bfloat16)
    return (mid + matmul(down_t[...], hidden)).astype(jnp.bfloat16)


def middle_kernel(
    product, pair, gate, out_t, up_t, down_t, gains, mask, proj, next_gains,
    edges, next_pair, next_gate, prod_scr, left_scr, right_scr,
):
    chunks, rows, channels = pair.shape[:3]
    for chunk in range(chunks):
        load_product(product, chunk, prod_scr)

        def step(row, carry):
            tri = take_row(prod_scr, row, rows, channels)
            new = finish_row(
                tri, pair[chunk, row].astype(jnp.float32), gate[chunk, row], out_t, up_t, down_t, gains
            )
            next_pair[chunk, row] = new
            next_gate[chunk, row] = edges_of_row(
                new.astype(jnp.float32), row, rows, mask[chunk, row], proj, next_gains[0],
                left_scr, right_scr,
            )
            return carry

        lax.fori_loop(0, rows, step, 0)
        write_edges(left_scr, right_scr, chunk, edges)


def last_kernel(product, pair, gate, out_t, up_t, down_t, gains, result, prod_scr):
    chunks, rows, channels = pair.shape[:3]
    for chunk in range(chunks):
        load_product(product, chunk, prod_scr)

        def step(row, carry):
            tri = take_row(prod_scr, row, rows, channels)
            new = finish_row(
                tri, pair[chunk, row].astype(jnp.float32), gate[chunk, row], out_t, up_t, down_t, gains
            )
            result[chunk, row] = new.astype(jnp.float32).T.astype(jnp.bfloat16)
            return carry

        lax.fori_loop(0, rows, step, 0)


def call(kernel, outs, scratch, *operands):
    whole = pl.BlockSpec(memory_space=pltpu.VMEM)
    return pl.pallas_call(
        kernel,
        out_shape=[jax.ShapeDtypeStruct(shape, dtype) for shape, dtype in outs],
        in_specs=[whole] * len(operands),
        out_specs=[whole] * len(outs),
        scratch_shapes=[pltpu.VMEM(shape, jnp.float32) for shape in scratch],
        compiler_params=pltpu.CompilerParams(vmem_limit_bytes=VMEM_BYTES),
    )(*operands)


def swap_parts(blocks, part, parts, width):
    if parts == 1:
        return blocks
    if parts == 2:
        size = parts * width
        arrived = lax.ppermute(
            jnp.where(part == 0, blocks[1], blocks[0]),
            "axial",
            [(i, (i + width) % size) for i in range(size)],
        )
        return jnp.stack(
            (jnp.where(part == 0, blocks[0], arrived), jnp.where(part == 0, arrived, blocks[1]))
        )
    groups = [[place + p * width for p in range(parts)] for place in range(width)]
    return lax.all_to_all(blocks, "axial", 0, 0, tiled=True, axis_index_groups=groups)


def per_layer(weight, section, sections):
    slots = [weight]
    for shift in range(1, sections):
        slots.append(
            lax.ppermute(weight, "section", [((i + shift) % sections, i) for i in range(sections)])
        )
    layers = []
    for layer in range(sections):
        chosen = slots[0]
        for shift in range(1, sections):
            chosen = jnp.where((section + shift) % sections == layer, slots[shift], chosen)
        layers.append(chosen)
    return layers


def per_device(pair_in, crop_mask, proj_weights, out_weights, up_weights, down_weights, norm_gains):
    section = lax.axis_index("section")
    sections = lax.axis_size("section")
    axial = lax.axis_size("axial")
    here = lax.axis_index("axial")
    own_count = pair_in.shape[0] // sections
    rows, columns, channels = pair_in.shape[1:]
    parts = own_count
    width = axial // parts
    per_group = channels // width
    block = per_group * rows
    part, place = here // width, here % width
    groups = [[p * width + i for i in range(width)] for p in range(parts)]
    own_pairs = lax.dynamic_slice_in_dim(pair_in, section * own_count, own_count, 0)
    current = swap_parts(own_pairs, part, parts, width)

    proj_t = proj_weights[0].transpose(0, 2, 1).reshape(-1, channels)
    heads = per_layer(jnp.concatenate((proj_t, norm_gains[0])), section, sections)
    middles = per_layer(
        jnp.concatenate((out_weights[0].T, up_weights[0].T)), section, sections
    )
    tails = per_layer(down_weights[0].T, section, sections)
    projs = [head[: 5 * channels] for head in heads]
    gains = [
        jnp.broadcast_to(head[5 * channels :].astype(jnp.float32)[:, :, None], (3, channels, columns))
        for head in heads
    ]
    outs = [middle[:channels] for middle in middles]
    ups = [middle[channels:] for middle in middles]

    mask_all = lax.dynamic_index_in_dim(
        crop_mask, section * own_count + part, 0, keepdims=False
    ).astype(jnp.float32)
    mask_rows = lax.dynamic_slice_in_dim(
        mask_all.reshape(parts, width, rows), place, 1, 1
    ).reshape(parts, rows)
    mask = (mask_rows[:, :, None] * mask_all)[:, :, None, :]

    tiles = columns // LANES
    wide_scr = (tiles, channels * rows, LANES)
    edges_out = ((width, parts, 2, block, columns), jnp.bfloat16)
    pair_out = ((parts, rows, channels, columns), jnp.bfloat16)
    gate_out = ((parts, rows, channels, columns), jnp.float32)
    exchange = functools.partial(
        lax.all_to_all, axis_name="axial", split_axis=0, concat_axis=0, tiled=True,
        axis_index_groups=groups,
    )
    edges, pair, gate = call(
        first_kernel, [edges_out, pair_out, gate_out], [wide_scr] * 2,
        current, mask, projs[0], gains[0],
    )
    for layer in range(sections):
        edges = exchange(edges)
        places = (parts * width, block, columns)
        (product,) = call(
            triangle_kernel, [((width, parts, block, columns), jnp.bfloat16)],
            [(2,) + places, places], edges,
        )
        product = exchange(product)
        shared = (product, pair, gate, outs[layer], ups[layer], tails[layer], gains[layer])
        if layer < sections - 1:
            edges, pair, gate = call(
                middle_kernel, [edges_out, pair_out, gate_out], [wide_scr] * 3,
                *shared, mask, projs[layer + 1], gains[layer + 1],
            )
        else:
            (result,) = call(
                last_kernel, [((parts, rows, columns, channels), jnp.bfloat16)], [wide_scr], *shared
            )
    return swap_parts(result, part, parts, width)


def solution(mesh):
    return jax.shard_map(
        per_device,
        mesh=mesh,
        in_specs=(
            P("groups", "axial", None, None),
            P("groups", None),
            P("section", None, None, None),
            P("section", None, None),
            P("section", None, None),
            P("section", None, None),
            P("section", None, None),
        ),
        out_specs=P(("groups", "section"), "axial", None, None),
        check_vma=False,
    )
```

```python
import functools

import jax
import jax.numpy as jnp
from jax import lax
from jax.experimental import pallas as pl
from jax.experimental.pallas import tpu as pltpu
from jax.sharding import PartitionSpec as P

epsilon = 1e-05
LANES = 128
TOGETHER = 1024
VMEM_BYTES = 48 * 1024 * 1024


def sigmoid(x):
    return 0.5 * jnp.tanh(0.5 * x) + 0.5


def normalize(values):
    count = values.shape[0]
    center = values - jnp.sum(values, axis=0, keepdims=True) * (1.0 / count)
    spread = jnp.sum(center * center, axis=0, keepdims=True) * (1.0 / count)
    return center * lax.rsqrt(spread + epsilon)


def matmul(a, b):
    return jnp.dot(a, b, preferred_element_type=jnp.float32)


def side_by_side(pieces):
    return pieces[0] if len(pieces) == 1 else jnp.concatenate(pieces, axis=1)


def put_rows(scratch, first, rows, values):
    tiles = scratch.shape[0]
    for place in range(values.shape[1] // LANES):
        scratch[place % tiles, pl.ds(first + place // tiles, values.shape[0], stride=rows), :] = (
            values[:, place * LANES : (place + 1) * LANES]
        )


def take_rows(scratch, first, count, rows, channels):
    return side_by_side(
        [
            scratch[tile, pl.ds(first + row, channels, stride=rows), :]
            for row in range(count)
            for tile in range(scratch.shape[0])
        ]
    )


def read_rows(ref, first, count):
    return side_by_side([ref[first + row] for row in range(count)])


def write_rows(ref, first, values):
    columns = ref.shape[-1]
    for row in range(values.shape[1] // columns):
        ref[first + row] = values[:, row * columns : (row + 1) * columns]


def edges_of_rows(pair_f, row, rows, mask, proj, gain, left_scr, right_scr):
    channels = pair_f.shape[0]
    normed = (normalize(pair_f) * gain).astype(jnp.bfloat16)
    linear = matmul(proj[...], normed)
    p0, p1, p2, p3, p4 = [linear[e * channels : (e + 1) * channels] for e in range(5)]
    put_rows(left_scr, row, rows, sigmoid(p1) * p0 * mask)
    put_rows(right_scr, row, rows, sigmoid(p3) * p2 * mask)
    return sigmoid(p4)


def write_edges(left_scr, right_scr, here, edges):
    block = edges[0].shape[2]
    for which, scr in enumerate((left_scr, right_scr)):
        for m in range(2 * len(edges)):
            start = pl.multiple_of((here[0] ^ m) * block, block)
            for tile in range(scr.shape[0]):
                edges[m // 2][m % 2, which, :, tile * LANES : (tile + 1) * LANES] = scr[
                    tile, pl.ds(start, block), :
                ].astype(jnp.bfloat16)


def arrived(own, cross, m):
    return cross[m // 2] if m % 2 else own[m // 2][0]


def repeat(gains, count):
    return side_by_side([gains] * count)


def rows_together(rows, columns):
    return min(rows, max(1, TOGETHER // columns))


def first_kernel(half, here, pair, mask, proj, gains, *refs):
    edges, (pair_t, gate, left_scr, right_scr) = refs[:half], refs[half:]
    rows, columns = pair.shape[:2]
    count = rows_together(rows, columns)

    def step(i, carry):
        row = i * count
        pair_f = side_by_side([pair[row + k].astype(jnp.float32).T for k in range(count)])
        write_rows(pair_t, row, pair_f.astype(jnp.bfloat16))
        opened = edges_of_rows(
            pair_f, row, rows, read_rows(mask, row, count), proj, repeat(gains[0], count),
            left_scr, right_scr,
        )
        write_rows(gate, row, opened)
        return carry

    lax.fori_loop(0, rows // count, step, 0)
    write_edges(left_scr, right_scr, here, edges)


def triangle_kernel(half, chunks, here, *refs):
    groups = 2 * half
    sources = [refs[k * (half + 1) : (k + 1) * (half + 1)] for k in range(chunks)]
    refs = refs[chunks * (half + 1) :]
    products = [refs[k * half : (k + 1) * half] for k in range(chunks)]
    wide, sums = refs[chunks * half :]
    block, columns = sums.shape[1:]
    places = groups * chunks
    rows = columns // places

    def place_of(k, m):
        return lax.rem(here[1] + k, chunks) * groups + (here[0] ^ m)

    for k in range(chunks):
        for m in range(groups):
            values = arrived(sources[k][:half], sources[k][half], m)
            for which in range(2):
                wide[which, place_of(k, m)] = values[which].astype(jnp.float32)

    def step(c, carry):
        at = pl.ds(pl.multiple_of(c * rows, rows), rows)
        left, right = [
            jnp.concatenate([wide[which, p, at, :] for p in range(places)], axis=0).astype(
                jnp.bfloat16
            )
            for which in range(2)
        ]
        total = lax.dot_general(
            left, right, (((1,), (1,)), ((), ())), preferred_element_type=jnp.float32
        )
        for p in range(places):
            sums[p, at, :] = total[p * rows : (p + 1) * rows]
        return carry

    lax.fori_loop(0, block // rows, step, 0, unroll=min(4, block // rows))
    for k in range(chunks):
        for m in range(groups):
            products[k][m // 2][m % 2] = sums[place_of(k, m)].astype(jnp.bfloat16)


def load_product(here, own, cross, prod_scr):
    block = cross.shape[1]
    for m in range(2 * len(own)):
        values = arrived(own, cross, m).astype(jnp.float32)
        start = pl.multiple_of((here[0] ^ m) * block, block)
        for tile in range(prod_scr.shape[0]):
            prod_scr[tile, pl.ds(start, block), :] = values[:, tile * LANES : (tile + 1) * LANES]


def finish_rows(prod_scr, row, count, pair, gate, out_t, up_t, down_t, gains):
    rows, channels = pair.shape[:2]
    tri = take_rows(prod_scr, row, count, rows, channels)
    tri_norm = (normalize(tri) * repeat(gains[1], count)).astype(jnp.bfloat16)
    mid = read_rows(pair, row, count).astype(jnp.float32) + read_rows(gate, row, count) * matmul(
        out_t[...], tri_norm
    )
    trans_in = (normalize(mid) * repeat(gains[2], count)).astype(jnp.bfloat16)
    hidden = jnp.maximum(matmul(up_t[...], trans_in), 0.0).astype(jnp.bfloat16)
    return (mid + matmul(down_t[...], hidden)).astype(jnp.bfloat16)


def middle_kernel(half, here, *refs):
    own, cross, refs = refs[:half], refs[half], refs[half + 1 :]
    pair, gate, out_t, up_t, down_t, gains, mask, proj, next_gains = refs[:9]
    edges, refs = refs[9 : 9 + half], refs[9 + half :]
    next_pair, next_gate, prod_scr, left_scr, right_scr = refs
    rows, _, columns = pair.shape
    count = rows_together(rows, columns)
    load_product(here, own, cross, prod_scr)

    def step(i, carry):
        row = i * count
        new = finish_rows(prod_scr, row, count, pair, gate, out_t, up_t, down_t, gains)
        write_rows(next_pair, row, new)
        opened = edges_of_rows(
            new.astype(jnp.float32), row, rows, read_rows(mask, row, count), proj,
            repeat(next_gains[0], count), left_scr, right_scr,
        )
        write_rows(next_gate, row, opened)
        return carry

    lax.fori_loop(0, rows // count, step, 0)
    write_edges(left_scr, right_scr, here, edges)


def last_kernel(half, here, *refs):
    own, cross, refs = refs[:half], refs[half], refs[half + 1 :]
    pair, gate, out_t, up_t, down_t, gains, result, prod_scr = refs
    rows, _, columns = pair.shape
    count = rows_together(rows, columns)
    load_product(here, own, cross, prod_scr)

    def step(i, carry):
        row = i * count
        new = finish_rows(prod_scr, row, count, pair, gate, out_t, up_t, down_t, gains)
        for k in range(count):
            result[row + k] = (
                new[:, k * columns : (k + 1) * columns].astype(jnp.float32).T.astype(jnp.bfloat16)
            )
        return carry

    lax.fori_loop(0, rows // count, step, 0)


def call(kernel, outs, scratch, flops, here, *operands):
    whole = pl.BlockSpec(memory_space=pltpu.VMEM)
    return pl.pallas_call(
        kernel,
        out_shape=[jax.ShapeDtypeStruct(shape, dtype) for shape, dtype in outs],
        in_specs=[pl.BlockSpec(memory_space=pltpu.SMEM)] + [whole] * len(operands),
        out_specs=[whole] * len(outs),
        scratch_shapes=[pltpu.VMEM(shape, jnp.float32) for shape in scratch],
        compiler_params=pltpu.CompilerParams(vmem_limit_bytes=VMEM_BYTES),
        cost_estimate=pl.CostEstimate(flops=flops, bytes_accessed=0, transcendentals=0),
    )(here, *operands)


def exchange(blocks, width, groups):
    half = len(blocks)
    if not by_permutes(width):
        whole = lax.all_to_all(
            jnp.concatenate(blocks), "axial", 0, 0, tiled=True, axis_index_groups=groups
        )
        return [whole[2 * i : 2 * i + 2] for i in range(half)], whole[1::2]
    size = lax.axis_size("axial")
    own = [blocks[0]] + [
        lax.ppermute(blocks[i], "axial", [(j, j ^ (2 * i)) for j in range(size)])
        for i in range(1, half)
    ]
    cross = lax.ppermute(
        jnp.stack([pair[1] for pair in own]), "axial", [(j, j ^ 1) for j in range(size)]
    )
    return own, cross


def by_permutes(width):
    return width in (2, 4, 8)


def move_parts(values, distance, width):
    if distance == 0:
        return values
    size = lax.axis_size("axial")
    return lax.ppermute(
        values, "axial", [(j, (j + distance * width) % size) for j in range(size)]
    )


def from_sections(weight, sections):
    return [weight] + [
        lax.ppermute(weight, "section", [((i + shift) % sections, i) for i in range(sections)])
        for shift in range(1, sections)
    ]


def by_layer(slots, section):
    sections = len(slots)
    layers = []
    for layer in range(sections):
        chosen = slots[0]
        for shift in range(1, sections):
            chosen = jnp.where((section + shift) % sections == layer, slots[shift], chosen)
        layers.append(chosen)
    return layers


def per_device(pair_in, crop_mask, proj_weights, out_weights, up_weights, down_weights, norm_gains):
    section = lax.axis_index("section")
    sections = lax.axis_size("section")
    axial = lax.axis_size("axial")
    own_count = pair_in.shape[0] // sections
    rows, columns, channels = pair_in.shape[1:]
    parts = own_count
    width = axial // parts
    half = width // 2
    block = channels // width * rows
    part, place = lax.axis_index("axial") // width, lax.axis_index("axial") % width
    groups = [[p * width + i for i in range(width)] for p in range(parts)]
    here = jnp.stack((place if by_permutes(width) else 0 * place, part)).astype(jnp.int32)

    pairs = [
        move_parts(
            lax.dynamic_index_in_dim(
                pair_in, section * own_count + (part + parts - k) % parts, 0, keepdims=False
            ),
            -k,
            width,
        )
        for k in range(parts)
    ]
    heads = from_sections(
        jnp.concatenate((proj_weights[0].transpose(0, 2, 1).reshape(-1, channels), norm_gains[0])),
        sections,
    )
    bodies = from_sections(jnp.concatenate((out_weights[0].T, up_weights[0].T)), sections)
    tails = from_sections(down_weights[0].T, sections)
    if parts > 1:
        pairs[-1], bodies, tails = lax.optimization_barrier((pairs[-1], bodies, tails))
    heads, bodies, tails = [by_layer(slots, section) for slots in (heads, bodies, tails)]
    projs = [head[: 5 * channels] for head in heads]
    gains = [
        jnp.broadcast_to(head[5 * channels :].astype(jnp.float32)[:, :, None], (3, channels, columns))
        for head in heads
    ]
    outs = [body[:channels] for body in bodies]
    ups = [body[channels:] for body in bodies]

    mask_all = lax.dynamic_index_in_dim(
        crop_mask, section * own_count + part, 0, keepdims=False
    ).astype(jnp.float32)
    masks = [
        (
            lax.dynamic_slice_in_dim(
                mask_all, ((part + k) % parts * width + place) * rows, rows
            )[:, None]
            * mask_all
        )[:, None, :]
        for k in range(parts)
    ]

    tiles = columns // LANES
    scratch = (tiles, channels * rows, LANES)
    edges_out = [((2, 2, block, columns), jnp.bfloat16)] * half
    state_out = [
        ((rows, channels, columns), jnp.bfloat16), ((rows, channels, columns), jnp.float32)
    ]
    hidden = ups[0].shape[0]
    points = rows * columns
    head_flops = 2 * points * 5 * channels * channels
    tail_flops = 2 * points * channels * (channels + 2 * hidden)
    edges, state = [None] * parts, [None] * parts
    for k in range(parts):
        *sent, pair, gate = call(
            functools.partial(first_kernel, half), edges_out + state_out, [scratch] * 2,
            head_flops, here, pairs[k], masks[k], projs[0], gains[0],
        )
        edges[k], state[k] = exchange(sent, width, groups), (pair, gate)
    result = None
    for layer in range(sections):
        places = (parts * width, block, columns)
        flat = [piece for own, cross in edges for piece in (*own, cross)]
        products = call(
            functools.partial(triangle_kernel, half, parts),
            [((2, block, columns), jnp.bfloat16)] * (half * parts), [(2,) + places, places],
            2 * channels // width * columns**3, here, *flat,
        )
        last = layer == sections - 1
        order = range(parts - 1, -1, -1) if last else range(parts)
        tri = {k: exchange(products[k * half : (k + 1) * half], width, groups) for k in order}
        for k in order:
            own, cross = tri[k]
            operands = (*own, cross, *state[k], outs[layer], ups[layer], tails[layer], gains[layer])
            if not last:
                *sent, pair, gate = call(
                    functools.partial(middle_kernel, half), edges_out + state_out, [scratch] * 3,
                    head_flops + tail_flops, here, *operands, masks[k], projs[layer + 1],
                    gains[layer + 1],
                )
                edges[k], state[k] = exchange(sent, width, groups), (pair, gate)
            else:
                (done,) = call(
                    functools.partial(last_kernel, half), [((rows, columns, channels), jnp.bfloat16)],
                    [scratch], tail_flops, here, *operands,
                )
                done = move_parts(done, k, width)[None]
                if result is None:
                    result = jnp.zeros((parts, rows, columns, channels), done.dtype)
                result = lax.dynamic_update_slice_in_dim(result, done, (part + parts - k) % parts, 0)
    return result


def solution(mesh):
    return jax.shard_map(
        per_device,
        mesh=mesh,
        in_specs=(
            P("groups", "axial", None, None),
            P("groups", None),
            P("section", None, None, None),
            P("section", None, None),
            P("section", None, None),
            P("section", None, None),
            P("section", None, None),
        ),
        out_specs=P(("groups", "section"), "axial", None, None),
        check_vma=False,
    )
```

```python
import functools

import jax
import jax.numpy as jnp
from jax import lax
from jax.experimental import pallas as pl
from jax.experimental.pallas import tpu as pltpu
from jax.sharding import PartitionSpec as P

epsilon = 1e-05
LANES = 128
TOGETHER = 1024
VMEM_BYTES = 48 * 1024 * 1024


def sigmoid(x):
    return 0.5 * jnp.tanh(0.5 * x) + 0.5


def normalize(values):
    count = values.shape[0]
    center = values - jnp.sum(values, axis=0, keepdims=True) * (1.0 / count)
    spread = jnp.sum(center * center, axis=0, keepdims=True) * (1.0 / count)
    return center * lax.rsqrt(spread + epsilon)


def matmul(a, b):
    return jnp.dot(a, b, preferred_element_type=jnp.float32)


def side_by_side(pieces):
    return pieces[0] if len(pieces) == 1 else jnp.concatenate(pieces, axis=1)


def put_rows(scratch, first, rows, values):
    tiles = scratch.shape[0]
    for place in range(values.shape[1] // LANES):
        scratch[place % tiles, pl.ds(first + place // tiles, values.shape[0], stride=rows), :] = (
            values[:, place * LANES : (place + 1) * LANES]
        )


def take_rows(scratch, first, count, rows, channels):
    return side_by_side(
        [
            scratch[tile, pl.ds(first + row, channels, stride=rows), :]
            for row in range(count)
            for tile in range(scratch.shape[0])
        ]
    )


def read_rows(ref, first, count):
    return side_by_side([ref[first + row] for row in range(count)])


def write_rows(ref, first, values):
    columns = ref.shape[-1]
    for row in range(values.shape[1] // columns):
        ref[first + row] = values[:, row * columns : (row + 1) * columns]


def edges_of_rows(pair_f, row, rows, mask, proj, gain, left_scr, right_scr):
    channels = pair_f.shape[0]
    normed = (normalize(pair_f) * gain).astype(jnp.bfloat16)
    linear = matmul(proj[...], normed)
    p0, p1, p2, p3, p4 = [linear[e * channels : (e + 1) * channels] for e in range(5)]
    put_rows(left_scr, row, rows, sigmoid(p1) * p0 * mask)
    put_rows(right_scr, row, rows, sigmoid(p3) * p2 * mask)
    return sigmoid(p4)


def write_edges(left_scr, right_scr, here, edges):
    block = edges[0].shape[2]
    for which, scr in enumerate((left_scr, right_scr)):
        for m in range(2 * len(edges)):
            start = pl.multiple_of((here[0] ^ m) * block, block)
            for tile in range(scr.shape[0]):
                edges[m // 2][m % 2, which, :, tile * LANES : (tile + 1) * LANES] = scr[
                    tile, pl.ds(start, block), :
                ].astype(jnp.bfloat16)


def arrived(own, cross, m):
    return cross[m // 2][1] if m % 2 else own[m // 2][0]


def repeat(gains, count):
    return side_by_side([gains] * count)


def rows_together(rows, columns):
    return min(rows, max(1, TOGETHER // columns))


def first_kernel(half, here, pair, mask, proj, gains, *refs):
    edges, (pair_t, gate, left_scr, right_scr) = refs[:half], refs[half:]
    rows, columns = pair.shape[:2]
    count = rows_together(rows, columns)

    def step(i, carry):
        row = i * count
        pair_f = side_by_side([pair[row + k].astype(jnp.float32).T for k in range(count)])
        write_rows(pair_t, row, pair_f.astype(jnp.bfloat16))
        opened = edges_of_rows(
            pair_f, row, rows, read_rows(mask, row, count), proj, repeat(gains[0], count),
            left_scr, right_scr,
        )
        write_rows(gate, row, opened)
        return carry

    lax.fori_loop(0, rows // count, step, 0)
    write_edges(left_scr, right_scr, here, edges)


def triangle_kernel(half, chunks, here, *refs):
    groups = 2 * half
    sources = [refs[k * groups : (k + 1) * groups] for k in range(chunks)]
    refs = refs[chunks * groups :]
    products = [refs[k * half : (k + 1) * half] for k in range(chunks)]
    wide, sums = refs[chunks * half :]
    block, columns = sums.shape[1:]
    places = groups * chunks
    rows = columns // places

    def place_of(k, m):
        return lax.rem(here[1] + k, chunks) * groups + (here[0] ^ m)

    for k in range(chunks):
        for m in range(groups):
            values = arrived(sources[k][:half], sources[k][half:], m)
            for which in range(2):
                wide[which, place_of(k, m)] = values[which].astype(jnp.float32)

    def step(c, carry):
        at = pl.ds(pl.multiple_of(c * rows, rows), rows)
        left, right = [
            jnp.concatenate([wide[which, p, at, :] for p in range(places)], axis=0).astype(
                jnp.bfloat16
            )
            for which in range(2)
        ]
        total = lax.dot_general(
            left, right, (((1,), (1,)), ((), ())), preferred_element_type=jnp.float32
        )
        for p in range(places):
            sums[p, at, :] = total[p * rows : (p + 1) * rows]
        return carry

    lax.fori_loop(0, block // rows, step, 0, unroll=min(4, block // rows))
    for k in range(chunks):
        for m in range(groups):
            products[k][m // 2][m % 2] = sums[place_of(k, m)].astype(jnp.bfloat16)


def load_product(here, own, cross, prod_scr):
    block = own[0].shape[1]
    for m in range(2 * len(own)):
        values = arrived(own, cross, m).astype(jnp.float32)
        start = pl.multiple_of((here[0] ^ m) * block, block)
        for tile in range(prod_scr.shape[0]):
            prod_scr[tile, pl.ds(start, block), :] = values[:, tile * LANES : (tile + 1) * LANES]


def finish_rows(prod_scr, row, count, pair, gate, out_t, up_t, down_t, gains):
    rows, channels = pair.shape[:2]
    tri = take_rows(prod_scr, row, count, rows, channels)
    tri_norm = (normalize(tri) * repeat(gains[1], count)).astype(jnp.bfloat16)
    mid = read_rows(pair, row, count).astype(jnp.float32) + read_rows(gate, row, count) * matmul(
        out_t[...], tri_norm
    )
    trans_in = (normalize(mid) * repeat(gains[2], count)).astype(jnp.bfloat16)
    hidden = jnp.maximum(matmul(up_t[...], trans_in), 0.0).astype(jnp.bfloat16)
    return (mid + matmul(down_t[...], hidden)).astype(jnp.bfloat16)


def middle_kernel(half, here, *refs):
    own, cross, refs = refs[:half], refs[half : 2 * half], refs[2 * half :]
    pair, gate, out_t, up_t, down_t, gains, mask, proj, next_gains = refs[:9]
    edges, refs = refs[9 : 9 + half], refs[9 + half :]
    next_pair, next_gate, prod_scr, left_scr, right_scr = refs
    rows, _, columns = pair.shape
    count = rows_together(rows, columns)
    load_product(here, own, cross, prod_scr)

    def step(i, carry):
        row = i * count
        new = finish_rows(prod_scr, row, count, pair, gate, out_t, up_t, down_t, gains)
        write_rows(next_pair, row, new)
        opened = edges_of_rows(
            new.astype(jnp.float32), row, rows, read_rows(mask, row, count), proj,
            repeat(next_gains[0], count), left_scr, right_scr,
        )
        write_rows(next_gate, row, opened)
        return carry

    lax.fori_loop(0, rows // count, step, 0)
    write_edges(left_scr, right_scr, here, edges)


def last_kernel(half, here, *refs):
    own, cross, refs = refs[:half], refs[half : 2 * half], refs[2 * half :]
    pair, gate, out_t, up_t, down_t, gains, result, prod_scr = refs
    rows, _, columns = pair.shape
    count = rows_together(rows, columns)
    slot = here[1] if result.shape[0] > 1 else 0
    load_product(here, own, cross, prod_scr)

    def step(i, carry):
        row = i * count
        new = finish_rows(prod_scr, row, count, pair, gate, out_t, up_t, down_t, gains)
        for k in range(count):
            result[slot, row + k] = (
                new[:, k * columns : (k + 1) * columns].astype(jnp.float32).T.astype(jnp.bfloat16)
            )
        return carry

    lax.fori_loop(0, rows // count, step, 0)


def call(kernel, outs, scratch, flops, here, *operands):
    whole = pl.BlockSpec(memory_space=pltpu.VMEM)
    return pl.pallas_call(
        kernel,
        out_shape=[jax.ShapeDtypeStruct(shape, dtype) for shape, dtype in outs],
        in_specs=[pl.BlockSpec(memory_space=pltpu.SMEM)] + [whole] * len(operands),
        out_specs=[whole] * len(outs),
        scratch_shapes=[pltpu.VMEM(shape, jnp.float32) for shape in scratch],
        compiler_params=pltpu.CompilerParams(vmem_limit_bytes=VMEM_BYTES),
        cost_estimate=pl.CostEstimate(flops=flops, bytes_accessed=0, transcendentals=0),
    )(here, *operands)


def exchange(blocks, width, groups):
    half = len(blocks)
    if not by_permutes(width):
        whole = lax.all_to_all(
            jnp.concatenate(blocks), "axial", 0, 0, tiled=True, axis_index_groups=groups
        )
        return [whole[2 * i : 2 * i + 2] for i in range(half)] * 2
    size = lax.axis_size("axial")
    own = [blocks[0]] + [
        lax.ppermute(blocks[i], "axial", [(j, j ^ (2 * i)) for j in range(size)])
        for i in range(1, half)
    ]
    return own + [lax.ppermute(pair, "axial", [(j, j ^ 1) for j in range(size)]) for pair in own]


def by_permutes(width):
    return width in (2, 4, 8)


def move_parts(values, distance, width):
    if distance == 0:
        return values
    size = lax.axis_size("axial")
    return lax.ppermute(
        values, "axial", [(j, (j + distance * width) % size) for j in range(size)]
    )


def from_sections(weight, sections):
    return [weight] + [
        lax.ppermute(weight, "section", [((i + shift) % sections, i) for i in range(sections)])
        for shift in range(1, sections)
    ]


def by_layer(slots, section):
    sections = len(slots)
    layers = []
    for layer in range(sections):
        chosen = slots[0]
        for shift in range(1, sections):
            chosen = jnp.where((section + shift) % sections == layer, slots[shift], chosen)
        layers.append(chosen)
    return layers


def per_device(pair_in, crop_mask, proj_weights, out_weights, up_weights, down_weights, norm_gains):
    section = lax.axis_index("section")
    sections = lax.axis_size("section")
    axial = lax.axis_size("axial")
    own_count = pair_in.shape[0] // sections
    rows, columns, channels = pair_in.shape[1:]
    parts = own_count
    width = axial // parts
    half = width // 2
    block = channels // width * rows
    part, place = lax.axis_index("axial") // width, lax.axis_index("axial") % width
    groups = [[p * width + i for i in range(width)] for p in range(parts)]
    here = jnp.stack((place if by_permutes(width) else 0 * place, part)).astype(jnp.int32)

    pairs = [
        move_parts(
            lax.dynamic_index_in_dim(
                pair_in, section * own_count + (part + parts - k) % parts, 0, keepdims=False
            ),
            -k,
            width,
        )
        for k in range(parts)
    ]
    projs, gains = [from_sections(w[0], sections) for w in (proj_weights, norm_gains)]
    others = (out_weights[0], up_weights[0], down_weights[0])
    *others, projs[-1] = lax.optimization_barrier((*others, projs[-1]))
    others = [from_sections(w, sections) for w in others]
    pairs[-1], others = lax.optimization_barrier((pairs[-1], others))
    projs = [w.transpose(0, 2, 1).reshape(-1, channels) for w in by_layer(projs, section)]
    outs, ups, downs = [[w.T for w in by_layer(slots, section)] for slots in others]
    gains = [
        jnp.broadcast_to(g.astype(jnp.float32)[:, :, None], g.shape + (columns,))
        for g in by_layer(gains, section)
    ]

    mask_all = lax.dynamic_index_in_dim(
        crop_mask, section * own_count + part, 0, keepdims=False
    ).astype(jnp.float32)
    masks = [
        (
            lax.dynamic_slice_in_dim(
                mask_all, ((part + k) % parts * width + place) * rows, rows
            )[:, None]
            * mask_all
        )[:, None, :]
        for k in range(parts)
    ]

    tiles = columns // LANES
    scratch = (tiles, channels * rows, LANES)
    edges_out = [((2, 2, block, columns), jnp.bfloat16)] * half
    state_out = [
        ((rows, channels, columns), jnp.bfloat16), ((rows, channels, columns), jnp.float32)
    ]
    hidden = ups[0].shape[0]
    points = rows * columns
    head_flops = 2 * points * 5 * channels * channels
    tail_flops = 2 * points * channels * (channels + 2 * hidden)
    edges, state = [None] * parts, [None] * parts
    for k in range(parts):
        *sent, pair, gate = call(
            functools.partial(first_kernel, half), edges_out + state_out, [scratch] * 2,
            head_flops, here, pairs[k], masks[k], projs[0], gains[0],
        )
        edges[k], state[k] = exchange(sent, width, groups), (pair, gate)
    finished = [None] * parts
    for layer in range(sections):
        places = (parts * width, block, columns)
        products = call(
            functools.partial(triangle_kernel, half, parts),
            [((2, block, columns), jnp.bfloat16)] * (half * parts), [(2,) + places, places],
            2 * channels // width * columns**3, here, *sum(edges, []),
        )
        last = layer == sections - 1
        order = range(parts - 1, -1, -1) if last else range(parts)
        tri = {k: exchange(products[k * half : (k + 1) * half], width, groups) for k in order}
        for k in order:
            operands = (*tri[k], *state[k], outs[layer], ups[layer], downs[layer], gains[layer])
            if not last:
                *sent, pair, gate = call(
                    functools.partial(middle_kernel, half), edges_out + state_out, [scratch] * 3,
                    head_flops + tail_flops, here, *operands, masks[k], projs[layer + 1],
                    gains[layer + 1],
                )
                edges[k], state[k] = exchange(sent, width, groups), (pair, gate)
            else:
                slots = 1 if k else parts
                (done,) = call(
                    functools.partial(last_kernel, half),
                    [((slots, rows, columns, channels), jnp.bfloat16)],
                    [scratch], tail_flops, here, *operands,
                )
                finished[k] = move_parts(done, k, width)
    result = finished[0]
    for k in range(1, parts):
        result = lax.dynamic_update_slice_in_dim(result, finished[k], (part + parts - k) % parts, 0)
    return result


def solution(mesh):
    return jax.shard_map(
        per_device,
        mesh=mesh,
        in_specs=(
            P("groups", "axial", None, None),
            P("groups", None),
            P("section", None, None, None),
            P("section", None, None),
            P("section", None, None),
            P("section", None, None),
            P("section", None, None),
        ),
        out_specs=P(("groups", "section"), "axial", None, None),
        check_vma=False,
    )
```

```python
import functools

import jax
import jax.numpy as jnp
from jax import lax
from jax.experimental import pallas as pl
from jax.experimental.pallas import tpu as pltpu
from jax.sharding import PartitionSpec as P


epsilon = 1e-05
LANES = 128
TOGETHER = 1024
VMEM_BYTES = 48 * 1024 * 1024


def sigmoid(x):
    return 0.5 * jnp.tanh(0.5 * x) + 0.5


def normalize(values):
    count = values.shape[0]
    center = values - jnp.sum(values, axis=0, keepdims=True) * (1.0 / count)
    spread = jnp.sum(center * center, axis=0, keepdims=True) * (1.0 / count)
    return center * lax.rsqrt(spread + epsilon)


def matmul(a, b):
    return jnp.dot(a, b, preferred_element_type=jnp.float32)


def side_by_side(pieces):
    return pieces[0] if len(pieces) == 1 else jnp.concatenate(pieces, axis=1)


def put_rows(scratch, first, rows, values):
    tiles = scratch.shape[0]
    for place in range(values.shape[1] // LANES):
        scratch[place % tiles, pl.ds(first + place // tiles, values.shape[0], stride=rows), :] = (
            values[:, place * LANES : (place + 1) * LANES]
        )


def take_rows(scratch, first, count, rows, channels):
    return side_by_side(
        [
            scratch[tile, pl.ds(first + row, channels, stride=rows), :]
            for row in range(count)
            for tile in range(scratch.shape[0])
        ]
    )


def read_rows(ref, first, count):
    return side_by_side([ref[first + row] for row in range(count)])


def write_rows(ref, first, values):
    columns = ref.shape[-1]
    for row in range(values.shape[1] // columns):
        ref[first + row] = values[:, row * columns : (row + 1) * columns]


def edges_of_rows(pair_f, row, rows, mask, proj, gain, left_scr, right_scr):
    channels = pair_f.shape[0]
    normed = (normalize(pair_f) * gain).astype(jnp.bfloat16)
    linear = matmul(proj[...], normed)
    p0, p1, p2, p3, p4 = [linear[e * channels : (e + 1) * channels] for e in range(5)]
    put_rows(left_scr, row, rows, sigmoid(p1) * p0 * mask)
    put_rows(right_scr, row, rows, sigmoid(p3) * p2 * mask)
    return sigmoid(p4)


def write_edges(left_scr, right_scr, here, edges):
    block = edges[0].shape[2]
    for which, scr in enumerate((left_scr, right_scr)):
        for m in range(2 * len(edges)):
            start = pl.multiple_of((here[0] ^ m) * block, block)
            for tile in range(scr.shape[0]):
                edges[m // 2][m % 2, which, :, tile * LANES : (tile + 1) * LANES] = scr[
                    tile, pl.ds(start, block), :
                ].astype(jnp.bfloat16)


def arrived(own, cross, m):
    return cross[m // 2][1] if m % 2 else own[m // 2][0]


def repeat(gains, count):
    return side_by_side([gains] * count)


def rows_together(rows, columns):
    return min(rows, max(1, TOGETHER // columns))


def first_kernel(half, here, pair, mask, proj, gains, *refs):
    edges, (pair_t, gate, left_scr, right_scr) = refs[:half], refs[half:]
    rows, columns = pair.shape[:2]
    count = rows_together(rows, columns)

    def step(i, carry):
        row = i * count
        pair_f = side_by_side([pair[row + k].astype(jnp.float32).T for k in range(count)])
        write_rows(pair_t, row, pair_f.astype(jnp.bfloat16))
        opened = edges_of_rows(
            pair_f, row, rows, read_rows(mask, row, count), proj, repeat(gains[0], count),
            left_scr, right_scr,
        )
        write_rows(gate, row, opened)
        return carry

    lax.fori_loop(0, rows // count, step, 0)
    write_edges(left_scr, right_scr, here, edges)


def triangle_kernel(half, chunks, here, *refs):
    groups = 2 * half
    sources = [refs[k * groups : (k + 1) * groups] for k in range(chunks)]
    refs = refs[chunks * groups :]
    products = [refs[k * half : (k + 1) * half] for k in range(chunks)]
    wide, sums = refs[chunks * half :]
    block, columns = sums.shape[1:]
    places = groups * chunks
    rows = columns // places

    def place_of(k, m):
        return lax.rem(here[1] + k, chunks) * groups + (here[0] ^ m)

    for k in range(chunks):
        for m in range(groups):
            values = arrived(sources[k][:half], sources[k][half:], m)
            for which in range(2):
                wide[which, place_of(k, m)] = values[which].astype(jnp.float32)

    def step(c, carry):
        at = pl.ds(pl.multiple_of(c * rows, rows), rows)
        left, right = [
            jnp.concatenate([wide[which, p, at, :] for p in range(places)], axis=0).astype(
                jnp.bfloat16
            )
            for which in range(2)
        ]
        total = lax.dot_general(
            left, right, (((1,), (1,)), ((), ())), preferred_element_type=jnp.float32
        )
        for p in range(places):
            sums[p, at, :] = total[p * rows : (p + 1) * rows]
        return carry

    lax.fori_loop(0, block // rows, step, 0, unroll=min(4, block // rows))
    for k in range(chunks):
        for m in range(groups):
            products[k][m // 2][m % 2] = sums[place_of(k, m)].astype(jnp.bfloat16)


def load_product(here, own, cross, prod_scr):
    block = own[0].shape[1]
    for m in range(2 * len(own)):
        values = arrived(own, cross, m).astype(jnp.float32)
        start = pl.multiple_of((here[0] ^ m) * block, block)
        for tile in range(prod_scr.shape[0]):
            prod_scr[tile, pl.ds(start, block), :] = values[:, tile * LANES : (tile + 1) * LANES]


def finish_rows(prod_scr, row, count, pair, gate, out_t, up_t, down_t, gains):
    rows, channels = pair.shape[:2]
    tri = take_rows(prod_scr, row, count, rows, channels)
    tri_norm = (normalize(tri) * repeat(gains[1], count)).astype(jnp.bfloat16)
    mid = read_rows(pair, row, count).astype(jnp.float32) + read_rows(gate, row, count) * matmul(
        out_t[...], tri_norm
    )
    trans_in = (normalize(mid) * repeat(gains[2], count)).astype(jnp.bfloat16)
    hidden = jnp.maximum(matmul(up_t[...], trans_in), 0.0).astype(jnp.bfloat16)
    return (mid + matmul(down_t[...], hidden)).astype(jnp.bfloat16)


def middle_kernel(half, here, *refs):
    own, cross, refs = refs[:half], refs[half : 2 * half], refs[2 * half :]
    pair, gate, out_t, up_t, down_t, gains, mask, proj, next_gains = refs[:9]
    edges, refs = refs[9 : 9 + half], refs[9 + half :]
    next_pair, next_gate, prod_scr, left_scr, right_scr = refs
    rows, _, columns = pair.shape
    count = rows_together(rows, columns)
    load_product(here, own, cross, prod_scr)

    def step(i, carry):
        row = i * count
        new = finish_rows(prod_scr, row, count, pair, gate, out_t, up_t, down_t, gains)
        write_rows(next_pair, row, new)
        opened = edges_of_rows(
            new.astype(jnp.float32), row, rows, read_rows(mask, row, count), proj,
            repeat(next_gains[0], count), left_scr, right_scr,
        )
        write_rows(next_gate, row, opened)
        return carry

    lax.fori_loop(0, rows // count, step, 0)
    write_edges(left_scr, right_scr, here, edges)


def last_kernel(half, here, *refs):
    own, cross, refs = refs[:half], refs[half : 2 * half], refs[2 * half :]
    pair, gate, out_t, up_t, down_t, gains, result, prod_scr = refs
    rows, _, columns = pair.shape
    count = rows_together(rows, columns)
    slot = here[1] if result.shape[0] > 1 else 0
    load_product(here, own, cross, prod_scr)

    def step(i, carry):
        row = i * count
        new = finish_rows(prod_scr, row, count, pair, gate, out_t, up_t, down_t, gains)
        for k in range(count):
            result[slot, row + k] = (
                new[:, k * columns : (k + 1) * columns].astype(jnp.float32).T.astype(jnp.bfloat16)
            )
        return carry

    lax.fori_loop(0, rows // count, step, 0)


def call(kernel, outs, scratch, flops, here, *operands):
    whole = pl.BlockSpec(memory_space=pltpu.VMEM)
    return pallas(kernel, outs, scratch, flops, whole, here, *operands)


def pallas(kernel, outs, scratch, flops, whole, here, *operands):
    return pl.pallas_call(
        kernel,
        out_shape=[jax.ShapeDtypeStruct(shape, dtype) for shape, dtype in outs],
        in_specs=[pl.BlockSpec(memory_space=pltpu.SMEM)] + [whole] * len(operands),
        out_specs=[whole] * len(outs),
        scratch_shapes=[pltpu.VMEM(shape, jnp.float32) for shape in scratch],
        compiler_params=pltpu.CompilerParams(vmem_limit_bytes=VMEM_BYTES),
        cost_estimate=pl.CostEstimate(flops=flops, bytes_accessed=0, transcendentals=0),
    )(here, *operands)


def exchange(blocks, width, groups):
    half = len(blocks)
    if not by_permutes(width):
        whole = lax.all_to_all(
            jnp.concatenate(blocks), "axial", 0, 0, tiled=True, axis_index_groups=groups
        )
        return [whole[2 * i : 2 * i + 2] for i in range(half)] * 2
    size = lax.axis_size("axial")
    own = list(blocks)
    for i in range(half - 1, 0, -1):
        own[i] = lax.ppermute(blocks[i], "axial", [(j, j ^ (2 * i)) for j in range(size)])
    return own + [lax.ppermute(pair, "axial", [(j, j ^ 1) for j in range(size)]) for pair in own]


def by_permutes(width):
    return width in (2, 4, 8)


def move_parts(values, distance, width):
    if distance == 0:
        return values
    size = lax.axis_size("axial")
    return lax.ppermute(
        values, "axial", [(j, (j + distance * width) % size) for j in range(size)]
    )


def from_sections(weight, sections):
    return [weight] + [
        lax.ppermute(weight, "section", [((i + shift) % sections, i) for i in range(sections)])
        for shift in range(1, sections)
    ]


def by_layer(slots, section):
    sections = len(slots)
    layers = []
    for layer in range(sections):
        chosen = slots[0]
        for shift in range(1, sections):
            chosen = jnp.where((section + shift) % sections == layer, slots[shift], chosen)
        layers.append(chosen)
    return layers


def per_device(pair_in, crop_mask, proj_weights, out_weights, up_weights, down_weights, norm_gains):
    section = lax.axis_index("section")
    sections = lax.axis_size("section")
    axial = lax.axis_size("axial")
    own_count = pair_in.shape[0] // sections
    rows, columns, channels = pair_in.shape[1:]
    parts = own_count
    width = axial // parts
    half = width // 2
    block = channels // width * rows
    part, place = lax.axis_index("axial") // width, lax.axis_index("axial") % width
    groups = [[p * width + i for i in range(width)] for p in range(parts)]
    here = jnp.stack((place if by_permutes(width) else 0 * place, part)).astype(jnp.int32)

    pairs = []
    for k in range(parts):
        crop = lax.dynamic_index_in_dim(
            pair_in, section * own_count + (part + parts - k) % parts, 0, keepdims=False
        )
        pairs.append(move_parts(crop, -k, width))
    projs, gains = [from_sections(w[0], sections) for w in (proj_weights, norm_gains)]
    others = (out_weights[0], up_weights[0], down_weights[0])
    *others, projs[-1] = lax.optimization_barrier((*others, projs[-1]))
    others = [from_sections(w, sections) for w in others]
    pairs[-1], others = lax.optimization_barrier((pairs[-1], others))
    projs = [w.transpose(0, 2, 1).reshape(-1, channels) for w in by_layer(projs, section)]
    outs, ups, downs = [[w.T for w in by_layer(slots, section)] for slots in others]
    gains = [
        jnp.broadcast_to(g.astype(jnp.float32)[:, :, None], g.shape + (columns,))
        for g in by_layer(gains, section)
    ]

    mask_all = lax.dynamic_index_in_dim(
        crop_mask, section * own_count + part, 0, keepdims=False
    ).astype(jnp.float32)
    masks = [
        (
            lax.dynamic_slice_in_dim(
                mask_all, ((part + k) % parts * width + place) * rows, rows
            )[:, None]
            * mask_all
        )[:, None, :]
        for k in range(parts)
    ]

    tiles = columns // LANES
    scratch = (tiles, channels * rows, LANES)
    edges_out = [((2, 2, block, columns), jnp.bfloat16)] * half
    state_out = [
        ((rows, channels, columns), jnp.bfloat16), ((rows, channels, columns), jnp.float32)
    ]
    hidden = ups[0].shape[0]
    points = rows * columns
    head_flops = 2 * points * 5 * channels * channels
    tail_flops = 2 * points * channels * (channels + 2 * hidden)
    edges, state = [None] * parts, [None] * parts
    for k in range(parts):
        *sent, pair, gate = call(
            functools.partial(first_kernel, half), edges_out + state_out, [scratch] * 2,
            head_flops, here, pairs[k], masks[k], projs[0], gains[0],
        )
        edges[k], state[k] = exchange(sent, width, groups), (pair, gate)
    finished = [None] * parts
    for layer in range(sections):
        places = (parts * width, block, columns)
        products = call(
            functools.partial(triangle_kernel, half, parts),
            [((2, block, columns), jnp.bfloat16)] * (half * parts), [(2,) + places, places],
            2 * channels // width * columns**3, here, *sum(edges, []),
        )
        last = layer == sections - 1
        order = range(parts - 1, -1, -1) if last else range(parts)
        tri = {k: exchange(products[k * half : (k + 1) * half], width, groups) for k in order}
        for k in order:
            operands = (*tri[k], *state[k], outs[layer], ups[layer], downs[layer], gains[layer])
            if not last:
                *sent, pair, gate = call(
                    functools.partial(middle_kernel, half), edges_out + state_out, [scratch] * 3,
                    head_flops + tail_flops, here, *operands, masks[k], projs[layer + 1],
                    gains[layer + 1],
                )
                edges[k] = exchange(sent, width, groups)
                state[k] = (pair, gate)
            else:
                slots = 1 if k else parts
                (done,) = call(
                    functools.partial(last_kernel, half),
                    [((slots, rows, columns, channels), jnp.bfloat16)],
                    [scratch], tail_flops, here, *operands,
                )
                finished[k] = move_parts(done, k, width)
    result = finished[0]
    for k in range(1, parts):
        result = lax.dynamic_update_slice_in_dim(result, finished[k], (part + parts - k) % parts, 0)
    return result


def solution(mesh):
    def step(pair_in, *operands):
        mapped = jax.shard_map(
            per_device,
            mesh=mesh,
            in_specs=(
                P("groups", "axial", None, None),
                P("groups", None),
                P("section", None, None, None),
                P("section", None, None),
                P("section", None, None),
                P("section", None, None),
                P("section", None, None),
            ),
            out_specs=P(("groups", "section"), "axial", None, None),
            check_vma=False,
        )
        return mapped(pair_in, *operands)

    return step
```

```python
import functools

import jax
import jax.numpy as jnp
from jax import lax
from jax.experimental import pallas as pl
from jax.experimental.pallas import tpu as pltpu
from jax.sharding import PartitionSpec as P


epsilon = 1e-05
LANES = 128
TOGETHER = 1024
VMEM_BYTES = 24 * 1024 * 1024


def sigmoid(x):
    return 0.5 * jnp.tanh(0.5 * x) + 0.5


def normalize(values):
    count = values.shape[0]
    center = values - jnp.sum(values, axis=0, keepdims=True) * (1.0 / count)
    spread = jnp.sum(center * center, axis=0, keepdims=True) * (1.0 / count)
    return center * lax.rsqrt(spread + epsilon)


def matmul(a, b):
    return jnp.dot(a, b, preferred_element_type=jnp.float32)


def side_by_side(pieces):
    return pieces[0] if len(pieces) == 1 else jnp.concatenate(pieces, axis=1)


def put_rows(scratch, first, rows, values):
    tiles = scratch.shape[0]
    for place in range(values.shape[1] // LANES):
        scratch[place % tiles, pl.ds(first + place // tiles, values.shape[0], stride=rows), :] = (
            values[:, place * LANES : (place + 1) * LANES]
        )


def take_rows(scratch, first, count, rows, channels):
    return side_by_side(
        [
            scratch[tile, pl.ds(first + row, channels, stride=rows), :]
            for row in range(count)
            for tile in range(scratch.shape[0])
        ]
    )


def read_rows(ref, first, count):
    return side_by_side([ref[first + row] for row in range(count)])


def write_rows(ref, first, values):
    columns = ref.shape[-1]
    for row in range(values.shape[1] // columns):
        ref[first + row] = values[:, row * columns : (row + 1) * columns]


def edges_of_rows(pair_f, row, rows, mask, proj, gain, left_scr, right_scr):
    channels = pair_f.shape[0]
    normed = (normalize(pair_f) * gain).astype(jnp.bfloat16)
    linear = matmul(proj[...], normed)
    p0, p1, p2, p3, p4 = [linear[e * channels : (e + 1) * channels] for e in range(5)]
    put_rows(left_scr, row, rows, sigmoid(p1) * p0 * mask)
    put_rows(right_scr, row, rows, sigmoid(p3) * p2 * mask)
    return sigmoid(p4)


def write_edges(left_scr, right_scr, here, edges):
    block = edges[0].shape[2]
    for which, scr in enumerate((left_scr, right_scr)):
        for m in range(2 * len(edges)):
            start = pl.multiple_of((here[0] ^ m) * block, block)
            for tile in range(scr.shape[0]):
                edges[m // 2][m % 2, which, :, tile * LANES : (tile + 1) * LANES] = scr[
                    tile, pl.ds(start, block), :
                ].astype(jnp.bfloat16)


def arrived(own, cross, m):
    return cross[m // 2][1] if m % 2 else own[m // 2][0]


def repeat(gains, count):
    return side_by_side([gains] * count)


def rows_together(rows, columns):
    return min(rows, max(1, TOGETHER // columns))


def first_kernel(half, here, pair, mask, proj, gains, *refs):
    edges, (pair_t, gate, left_scr, right_scr) = refs[:half], refs[half:]
    rows, columns = pair.shape[:2]
    count = rows_together(rows, columns)

    def step(i, carry):
        row = i * count
        pair_f = side_by_side([pair[row + k].astype(jnp.float32).T for k in range(count)])
        write_rows(pair_t, row, pair_f.astype(jnp.bfloat16))
        opened = edges_of_rows(
            pair_f, row, rows, read_rows(mask, row, count), proj, repeat(gains[0], count),
            left_scr, right_scr,
        )
        write_rows(gate, row, opened.astype(jnp.bfloat16))
        return carry

    lax.fori_loop(0, rows // count, step, 0)
    write_edges(left_scr, right_scr, here, edges)


def triangle_kernel(half, chunks, here, *refs):
    groups = 2 * half
    sources = [refs[k * groups : (k + 1) * groups] for k in range(chunks)]
    refs = refs[chunks * groups :]
    products = [refs[k * half : (k + 1) * half] for k in range(chunks)]
    wide, sums = refs[chunks * half :]
    block, columns = sums.shape[1:]
    places = groups * chunks
    rows = columns // places

    def place_of(k, m):
        return lax.rem(here[1] + k, chunks) * groups + (here[0] ^ m)

    for k in range(chunks):
        for m in range(groups):
            values = arrived(sources[k][:half], sources[k][half:], m)
            for which in range(2):
                wide[which, place_of(k, m)] = values[which].astype(jnp.float32)

    def step(c, carry):
        at = pl.ds(pl.multiple_of(c * rows, rows), rows)
        left, right = [
            jnp.concatenate([wide[which, p, at, :] for p in range(places)], axis=0).astype(
                jnp.bfloat16
            )
            for which in range(2)
        ]
        total = lax.dot_general(
            left, right, (((1,), (1,)), ((), ())), preferred_element_type=jnp.float32
        )
        for p in range(places):
            sums[p, at, :] = total[p * rows : (p + 1) * rows]
        return carry

    lax.fori_loop(0, block // rows, step, 0, unroll=min(4, block // rows))
    for k in range(chunks):
        for m in range(groups):
            products[k][m // 2][m % 2] = sums[place_of(k, m)].astype(jnp.bfloat16)


def load_product(here, own, cross, prod_scr):
    block = own[0].shape[1]
    for m in range(2 * len(own)):
        values = arrived(own, cross, m).astype(jnp.float32)
        start = pl.multiple_of((here[0] ^ m) * block, block)
        for tile in range(prod_scr.shape[0]):
            prod_scr[tile, pl.ds(start, block), :] = values[:, tile * LANES : (tile + 1) * LANES]


def finish_rows(prod_scr, row, count, pair, gate, out_t, up_t, down_t, gains):
    rows, channels = pair.shape[:2]
    tri = take_rows(prod_scr, row, count, rows, channels)
    tri_norm = (normalize(tri) * repeat(gains[1], count)).astype(jnp.bfloat16)
    opened = read_rows(gate, row, count).astype(jnp.float32)
    mid = read_rows(pair, row, count).astype(jnp.float32) + opened * matmul(out_t[...], tri_norm)
    trans_in = (normalize(mid) * repeat(gains[2], count)).astype(jnp.bfloat16)
    hidden = jnp.maximum(matmul(up_t[...], trans_in), 0.0).astype(jnp.bfloat16)
    return (mid + matmul(down_t[...], hidden)).astype(jnp.bfloat16)


def middle_kernel(half, here, *refs):
    own, cross, refs = refs[:half], refs[half : 2 * half], refs[2 * half :]
    pair, gate, out_t, up_t, down_t, gains, mask, proj, next_gains = refs[:9]
    edges, refs = refs[9 : 9 + half], refs[9 + half :]
    next_pair, next_gate, prod_scr, left_scr, right_scr = refs
    rows, _, columns = pair.shape
    count = rows_together(rows, columns)
    load_product(here, own, cross, prod_scr)

    def step(i, carry):
        row = i * count
        new = finish_rows(prod_scr, row, count, pair, gate, out_t, up_t, down_t, gains)
        write_rows(next_pair, row, new)
        opened = edges_of_rows(
            new.astype(jnp.float32), row, rows, read_rows(mask, row, count), proj,
            repeat(next_gains[0], count), left_scr, right_scr,
        )
        write_rows(next_gate, row, opened.astype(jnp.bfloat16))
        return carry

    lax.fori_loop(0, rows // count, step, 0)
    write_edges(left_scr, right_scr, here, edges)


def last_kernel(half, here, *refs):
    own, cross, refs = refs[:half], refs[half : 2 * half], refs[2 * half :]
    pair, gate, out_t, up_t, down_t, gains, result, prod_scr = refs
    rows, _, columns = pair.shape
    count = rows_together(rows, columns)
    slot = here[1] if result.shape[0] > 1 else 0
    load_product(here, own, cross, prod_scr)

    def step(i, carry):
        row = i * count
        new = finish_rows(prod_scr, row, count, pair, gate, out_t, up_t, down_t, gains)
        for k in range(count):
            result[slot, row + k] = (
                new[:, k * columns : (k + 1) * columns].astype(jnp.float32).T.astype(jnp.bfloat16)
            )
        return carry

    lax.fori_loop(0, rows // count, step, 0)


def call(kernel, outs, scratch, flops, here, *operands):
    whole = pl.BlockSpec(memory_space=pltpu.VMEM)
    return pallas(kernel, outs, scratch, flops, whole, here, *operands)


def pallas(kernel, outs, scratch, flops, whole, here, *operands):
    return pl.pallas_call(
        kernel,
        out_shape=[jax.ShapeDtypeStruct(shape, dtype) for shape, dtype in outs],
        in_specs=[pl.BlockSpec(memory_space=pltpu.SMEM)] + [whole] * len(operands),
        out_specs=[whole] * len(outs),
        scratch_shapes=[pltpu.VMEM(shape, jnp.float32) for shape in scratch],
        compiler_params=pltpu.CompilerParams(vmem_limit_bytes=VMEM_BYTES),
        cost_estimate=pl.CostEstimate(flops=flops, bytes_accessed=0, transcendentals=0),
    )(here, *operands)


def exchange(blocks, width, groups):
    half = len(blocks)
    if not by_permutes(width):
        whole = lax.all_to_all(
            jnp.concatenate(blocks), "axial", 0, 0, tiled=True, axis_index_groups=groups
        )
        return [whole[2 * i : 2 * i + 2] for i in range(half)] * 2
    size = lax.axis_size("axial")
    own = list(blocks)
    for i in range(1, half):
        own[i] = lax.ppermute(blocks[i], "axial", [(j, j ^ (2 * i)) for j in range(size)])
    return own + [lax.ppermute(pair, "axial", [(j, j ^ 1) for j in range(size)]) for pair in own]


def by_permutes(width):
    return width in (2, 4, 8)


def move_parts(values, distance, width):
    if distance == 0:
        return values
    size = lax.axis_size("axial")
    return lax.ppermute(
        values, "axial", [(j, (j + distance * width) % size) for j in range(size)]
    )


def from_sections(weight, sections):
    return [weight] + [
        lax.ppermute(weight, "section", [((i + shift) % sections, i) for i in range(sections)])
        for shift in range(1, sections)
    ]


def by_layer(slots, section):
    sections = len(slots)
    layers = []
    for layer in range(sections):
        chosen = slots[0]
        for shift in range(1, sections):
            chosen = jnp.where((section + shift) % sections == layer, slots[shift], chosen)
        layers.append(chosen)
    return layers


def per_device(pair_in, crop_mask, proj_weights, out_weights, up_weights, down_weights, norm_gains):
    section = lax.axis_index("section")
    sections = lax.axis_size("section")
    axial = lax.axis_size("axial")
    own_count = pair_in.shape[0] // sections
    rows, columns, channels = pair_in.shape[1:]
    parts = own_count
    width = axial // parts
    half = width // 2
    block = channels // width * rows
    part, place = lax.axis_index("axial") // width, lax.axis_index("axial") % width
    groups = [[p * width + i for i in range(width)] for p in range(parts)]
    here = jnp.stack((place if by_permutes(width) else 0 * place, part)).astype(jnp.int32)

    pairs = []
    for k in range(parts):
        crop = lax.dynamic_index_in_dim(
            pair_in, section * own_count + (part + parts - k) % parts, 0, keepdims=False
        )
        pairs.append(move_parts(crop, -k, width))
    projs = from_sections(proj_weights[0], sections)
    gains = from_sections(norm_gains[0], sections)
    others = (out_weights[0], up_weights[0], down_weights[0])
    *others, projs[-1] = lax.optimization_barrier((*others, projs[-1]))
    others = [from_sections(w, sections) for w in others]
    projs = [w.transpose(0, 2, 1).reshape(-1, channels) for w in by_layer(projs, section)]
    outs, ups, downs = [[w.T for w in by_layer(slots, section)] for slots in others]
    gains = [
        jnp.broadcast_to(g.astype(jnp.float32)[:, :, None], g.shape + (columns,))
        for g in by_layer(gains, section)
    ]

    mask_all = lax.dynamic_index_in_dim(
        crop_mask, section * own_count + part, 0, keepdims=False
    ).astype(jnp.float32)
    masks = [
        (
            lax.dynamic_slice_in_dim(
                mask_all, ((part + k) % parts * width + place) * rows, rows
            )[:, None]
            * mask_all
        )[:, None, :]
        for k in range(parts)
    ]

    tiles = columns // LANES
    scratch = (tiles, channels * rows, LANES)
    edges_out = [((2, 2, block, columns), jnp.bfloat16)] * half
    state_out = [
        ((rows, channels, columns), jnp.bfloat16), ((rows, channels, columns), jnp.bfloat16)
    ]
    hidden = ups[0].shape[0]
    points = rows * columns
    head_flops = 2 * points * 5 * channels * channels
    tail_flops = 2 * points * channels * (channels + 2 * hidden)
    edges, state = [None] * parts, [None] * parts
    for k in range(parts):
        *sent, pair, gate = call(
            functools.partial(first_kernel, half), edges_out + state_out, [scratch] * 2,
            head_flops, here, pairs[k], masks[k], projs[0], gains[0],
        )
        edges[k], state[k] = exchange(sent, width, groups), (pair, gate)
    finished = [None] * parts
    for layer in range(sections):
        places = (parts * width, block, columns)
        products = call(
            functools.partial(triangle_kernel, half, parts),
            [((2, block, columns), jnp.bfloat16)] * (half * parts), [(2,) + places, places],
            2 * channels // width * columns**3, here, *sum(edges, []),
        )
        last = layer == sections - 1
        order = range(parts - 1, -1, -1) if last else range(parts)
        tri = {k: exchange(products[k * half : (k + 1) * half], width, groups) for k in order}
        for k in order:
            operands = (*tri[k], *state[k], outs[layer], ups[layer], downs[layer], gains[layer])
            if not last:
                *sent, pair, gate = call(
                    functools.partial(middle_kernel, half), edges_out + state_out, [scratch] * 3,
                    head_flops + tail_flops, here, *operands, masks[k], projs[layer + 1],
                    gains[layer + 1],
                )
                edges[k] = exchange(sent, width, groups)
                state[k] = (pair, gate)
            else:
                slots = 1 if k else parts
                (done,) = call(
                    functools.partial(last_kernel, half),
                    [((slots, rows, columns, channels), jnp.bfloat16)],
                    [scratch], tail_flops, here, *operands,
                )
                finished[k] = move_parts(done, k, width)
    result = finished[0]
    for k in range(1, parts):
        result = lax.dynamic_update_slice_in_dim(result, finished[k], (part + parts - k) % parts, 0)
    return result


def solution(mesh):
    def step(pair_in, *operands):
        mapped = jax.shard_map(
            per_device,
            mesh=mesh,
            in_specs=(
                P("groups", "axial", None, None),
                P("groups", None),
                P("section", None, None, None),
                P("section", None, None),
                P("section", None, None),
                P("section", None, None),
                P("section", None, None),
            ),
            out_specs=P(("groups", "section"), "axial", None, None),
            check_vma=False,
        )
        return mapped(pair_in, *operands)

    return step
```

```python
import functools

import jax
import jax.numpy as jnp
from jax import lax
from jax.experimental import pallas as pl
from jax.experimental.pallas import tpu as pltpu
from jax.sharding import PartitionSpec as P


epsilon = 1e-05
LANES = 128
TOGETHER = 1024
UNROLL = 4
VMEM_BYTES = 24 * 1024 * 1024


def sigmoid(x):
    return 0.5 * jnp.tanh(0.5 * x) + 0.5


def normalize(values):
    count = values.shape[0]
    center = values - jnp.sum(values, axis=0, keepdims=True) * (1.0 / count)
    spread = jnp.sum(center * center, axis=0, keepdims=True) * (1.0 / count)
    return center * lax.rsqrt(spread + epsilon)


def matmul(a, b):
    return jnp.dot(a, b, preferred_element_type=jnp.float32)


def side_by_side(pieces):
    return pieces[0] if len(pieces) == 1 else jnp.concatenate(pieces, axis=1)


def put_rows(scratch, first, rows, values):
    tiles = scratch.shape[0]
    for place in range(values.shape[1] // LANES):
        scratch[place % tiles, pl.ds(first + place // tiles, values.shape[0], stride=rows), :] = (
            values[:, place * LANES : (place + 1) * LANES]
        )


def take_rows(scratch, first, count, rows, channels):
    return side_by_side(
        [
            scratch[tile, pl.ds(first + row, channels, stride=rows), :]
            for row in range(count)
            for tile in range(scratch.shape[0])
        ]
    )


def read_rows(ref, first, count):
    return side_by_side([ref[first + row] for row in range(count)])


def write_rows(ref, first, values):
    columns = ref.shape[-1]
    for row in range(values.shape[1] // columns):
        ref[first + row] = values[:, row * columns : (row + 1) * columns]


def edges_of_rows(pair_f, row, rows, mask, proj, gain, left_scr, right_scr):
    channels = pair_f.shape[0]
    normed = (normalize(pair_f) * gain).astype(jnp.bfloat16)
    linear = matmul(proj[...], normed)
    p0, p1, p2, p3, p4 = [linear[e * channels : (e + 1) * channels] for e in range(5)]
    put_rows(left_scr, row, rows, sigmoid(p1) * p0 * mask)
    put_rows(right_scr, row, rows, sigmoid(p3) * p2 * mask)
    return sigmoid(p4)


def write_edges(left_scr, right_scr, here, edges):
    block = edges[0].shape[1]
    for which, scr in enumerate((left_scr, right_scr)):
        for i, edge in enumerate(edges):
            start = pl.multiple_of((here[0] ^ i) * block, block)
            for tile in range(scr.shape[0]):
                edge[which, :, tile * LANES : (tile + 1) * LANES] = scr[
                    tile, pl.ds(start, block), :
                ].astype(jnp.bfloat16)


def repeat(gains, count):
    return side_by_side([gains] * count)


def rows_together(rows, columns):
    return min(rows, max(1, TOGETHER // columns))


def first_kernel(half, here, pair, mask, proj, gains, *refs):
    edges, (pair_t, gate, left_scr, right_scr) = refs[:half], refs[half:]
    rows, columns = pair.shape[:2]
    count = rows_together(rows, columns)

    def step(i, carry):
        row = i * count
        pair_f = side_by_side([pair[row + k].astype(jnp.float32).T for k in range(count)])
        write_rows(pair_t, row, pair_f.astype(jnp.bfloat16))
        opened = edges_of_rows(
            pair_f, row, rows, read_rows(mask, row, count), proj, repeat(gains[0], count),
            left_scr, right_scr,
        )
        write_rows(gate, row, opened.astype(jnp.bfloat16))
        return carry

    lax.fori_loop(0, rows // count, step, 0)
    write_edges(left_scr, right_scr, here, edges)


def triangle_kernel(half, chunks, here, *refs):
    sources = [refs[k * 2 * half : (k + 1) * 2 * half] for k in range(chunks)]
    refs = refs[chunks * 2 * half :]
    products = [refs[k * half : (k + 1) * half] for k in range(chunks)]
    lefts, rights, sums = refs[chunks * half :]
    block, columns = sums.shape[1:]
    places = 2 * half * chunks
    rows = columns // places
    for k in range(chunks):
        for i in range(half):
            chip = lax.rem(here[2] + k, chunks) * half + (here[0] ^ i)
            lefts[k * half + i] = sources[k][i][0].astype(jnp.float32)
            rights[2 * chip + here[1]] = sources[k][i][1].astype(jnp.float32)
            rights[2 * chip + 1 - here[1]] = sources[k][half + i][1].astype(jnp.float32)

    def step(c, carry):
        at = pl.ds(pl.multiple_of(c * rows, rows), rows)
        left, right = [
            jnp.concatenate([wide[p, at, :] for p in range(wide.shape[0])], axis=0).astype(
                jnp.bfloat16
            )
            for wide in (lefts, rights)
        ]
        total = lax.dot_general(
            left, right, (((1,), (1,)), ((), ())), preferred_element_type=jnp.float32
        )
        for p in range(half * chunks):
            sums[p, at, :] = total[p * rows : (p + 1) * rows]
        return carry

    lax.fori_loop(0, block // rows, step, 0, unroll=min(UNROLL, block // rows))
    for k in range(chunks):
        for i in range(half):
            products[k][i][...] = sums[k * half + i].astype(jnp.bfloat16)


def load_product(here, own, prod_scr):
    block = own[0].shape[0]
    for i, piece in enumerate(own):
        values = piece[...].astype(jnp.float32)
        start = pl.multiple_of((here[0] ^ i) * block, block)
        for tile in range(prod_scr.shape[0]):
            prod_scr[tile, pl.ds(start, block), :] = values[:, tile * LANES : (tile + 1) * LANES]


def finish_rows(prod_scr, row, count, pair, gate, out_t, up_t, down_t, gains):
    rows, channels = pair.shape[:2]
    tri = take_rows(prod_scr, row, count, rows, channels)
    tri_norm = (normalize(tri) * repeat(gains[1], count)).astype(jnp.bfloat16)
    opened = read_rows(gate, row, count).astype(jnp.float32)
    mid = read_rows(pair, row, count).astype(jnp.float32) + opened * matmul(out_t[...], tri_norm)
    trans_in = (normalize(mid) * repeat(gains[2], count)).astype(jnp.bfloat16)
    hidden = jnp.maximum(matmul(up_t[...], trans_in), 0.0).astype(jnp.bfloat16)
    return (mid + matmul(down_t[...], hidden)).astype(jnp.bfloat16)


def middle_kernel(half, here, *refs):
    own, refs = refs[:half], refs[half:]
    pair, gate, out_t, up_t, down_t, gains, mask, proj, next_gains = refs[:9]
    edges, refs = refs[9 : 9 + half], refs[9 + half :]
    next_pair, next_gate, prod_scr, left_scr, right_scr = refs
    rows, _, columns = pair.shape
    count = rows_together(rows, columns)
    load_product(here, own, prod_scr)

    def step(i, carry):
        row = i * count
        new = finish_rows(prod_scr, row, count, pair, gate, out_t, up_t, down_t, gains)
        write_rows(next_pair, row, new)
        opened = edges_of_rows(
            new.astype(jnp.float32), row, rows, read_rows(mask, row, count), proj,
            repeat(next_gains[0], count), left_scr, right_scr,
        )
        write_rows(next_gate, row, opened.astype(jnp.bfloat16))
        return carry

    lax.fori_loop(0, rows // count, step, 0)
    write_edges(left_scr, right_scr, here, edges)


def last_kernel(half, here, *refs):
    own, refs = refs[:half], refs[half:]
    pair, gate, out_t, up_t, down_t, gains, result, prod_scr = refs
    rows, _, columns = pair.shape
    count = rows_together(rows, columns)
    slot = here[2] if result.shape[0] > 1 else 0
    load_product(here, own, prod_scr)

    def step(i, carry):
        row = i * count
        new = finish_rows(prod_scr, row, count, pair, gate, out_t, up_t, down_t, gains)
        for k in range(count):
            result[slot, row + k] = (
                new[:, k * columns : (k + 1) * columns].astype(jnp.float32).T.astype(jnp.bfloat16)
            )
        return carry

    lax.fori_loop(0, rows // count, step, 0)


def call(kernel, outs, scratch, flops, here, *operands):
    whole = pl.BlockSpec(memory_space=pltpu.VMEM)
    return pallas(kernel, outs, scratch, flops, whole, here, *operands)


def pallas(kernel, outs, scratch, flops, whole, here, *operands):
    return pl.pallas_call(
        kernel,
        out_shape=[jax.ShapeDtypeStruct(shape, dtype) for shape, dtype in outs],
        in_specs=[pl.BlockSpec(memory_space=pltpu.SMEM)] + [whole] * len(operands),
        out_specs=[whole] * len(outs),
        scratch_shapes=[pltpu.VMEM(shape, jnp.float32) for shape in scratch],
        compiler_params=pltpu.CompilerParams(vmem_limit_bytes=VMEM_BYTES),
        cost_estimate=pl.CostEstimate(flops=flops, bytes_accessed=0, transcendentals=0),
    )(here, *operands)


def exchange(blocks, width, groups):
    half = len(blocks)
    if not by_permutes(width):
        whole = lax.all_to_all(
            jnp.stack(blocks), "axial", 0, 0, tiled=True, axis_index_groups=groups
        )
        return [whole[i] for i in range(half)]
    size = lax.axis_size("axial")
    own = list(blocks)
    for i in range(1, half):
        own[i] = lax.ppermute(blocks[i], "axial", [(j, j ^ (2 * i)) for j in range(size)])
    return own


def with_neighbour(own):
    swap = [(j, j ^ 1) for j in range(lax.axis_size("axial"))]
    if not by_permutes(2 * len(own)):
        whole = lax.ppermute(jnp.stack(own), "axial", swap)
        return own + [whole[i] for i in range(len(own))]
    return own + [lax.ppermute(piece, "axial", swap) for piece in own]


def by_permutes(width):
    return width in (2, 4, 8)


def move_parts(values, distance, width):
    if distance == 0:
        return values
    size = lax.axis_size("axial")
    return lax.ppermute(
        values, "axial", [(j, (j + distance * width) % size) for j in range(size)]
    )


def from_sections(weight, sections):
    return [weight] + [
        lax.ppermute(weight, "section", [((i + shift) % sections, i) for i in range(sections)])
        for shift in range(1, sections)
    ]


def by_layer(slots, section):
    sections = len(slots)
    layers = []
    for layer in range(sections):
        chosen = slots[0]
        for shift in range(1, sections):
            chosen = jnp.where((section + shift) % sections == layer, slots[shift], chosen)
        layers.append(chosen)
    return layers


def per_device(pair_in, crop_mask, proj_weights, out_weights, up_weights, down_weights, norm_gains):
    section = lax.axis_index("section")
    sections = lax.axis_size("section")
    axial = lax.axis_size("axial")
    own_count = pair_in.shape[0] // sections
    rows, columns, channels = pair_in.shape[1:]
    parts = own_count
    width = axial // parts
    half = width // 2
    block = channels // half * rows
    part, place = lax.axis_index("axial") // width, lax.axis_index("axial") % width
    groups = [
        [p * width + 2 * i + core for i in range(half)] for p in range(parts) for core in range(2)
    ]
    chip = place // 2 if by_permutes(width) else 0 * place
    here = jnp.stack((chip, place % 2, part)).astype(jnp.int32)

    pairs = []
    for k in range(parts):
        crop = lax.dynamic_index_in_dim(
            pair_in, section * own_count + (part + parts - k) % parts, 0, keepdims=False
        )
        pairs.append(move_parts(crop, -k, width))
    projs = from_sections(proj_weights[0], sections)
    gains = from_sections(norm_gains[0], sections)
    others = (out_weights[0], up_weights[0], down_weights[0])
    *others, projs[-1] = lax.optimization_barrier((*others, projs[-1]))
    others = [from_sections(w, sections) for w in others]
    projs = [w.transpose(0, 2, 1).reshape(-1, channels) for w in by_layer(projs, section)]
    outs, ups, downs = [[w.T for w in by_layer(slots, section)] for slots in others]
    gains = [
        jnp.broadcast_to(g.astype(jnp.float32)[:, :, None], g.shape + (columns,))
        for g in by_layer(gains, section)
    ]

    mask_all = lax.dynamic_index_in_dim(
        crop_mask, section * own_count + part, 0, keepdims=False
    ).astype(jnp.float32)
    masks = [
        (
            lax.dynamic_slice_in_dim(
                mask_all, ((part + k) % parts * width + place) * rows, rows
            )[:, None]
            * mask_all
        )[:, None, :]
        for k in range(parts)
    ]

    tiles = columns // LANES
    scratch = (tiles, channels * rows, LANES)
    edges_out = [((2, block, columns), jnp.bfloat16)] * half
    state_out = [
        ((rows, channels, columns), jnp.bfloat16), ((rows, channels, columns), jnp.bfloat16)
    ]
    hidden = ups[0].shape[0]
    points = rows * columns
    head_flops = 2 * points * 5 * channels * channels
    tail_flops = 2 * points * channels * (channels + 2 * hidden)
    edges, state = [None] * parts, [None] * parts
    for k in range(parts):
        *sent, pair, gate = call(
            functools.partial(first_kernel, half), edges_out + state_out, [scratch] * 2,
            head_flops, here, pairs[k], masks[k], projs[0], gains[0],
        )
        edges[k] = exchange(sent, width, groups)
        state[k] = (pair, gate)
    finished = [None] * parts
    for layer in range(sections):
        edges = [with_neighbour(edges[k]) for k in range(parts)]
        sides = [(n * parts * half, block, columns) for n in (1, 2, 1)]
        products = call(
            functools.partial(triangle_kernel, half, parts),
            [((block, columns), jnp.bfloat16)] * (half * parts), sides,
            2 * channels // width * columns**3, here, *sum(edges, []),
        )
        last = layer == sections - 1
        order = range(parts - 1, -1, -1) if last else range(parts)
        tri = {k: exchange(products[k * half : (k + 1) * half], width, groups) for k in order}
        for k in order:
            operands = (*tri[k], *state[k], outs[layer], ups[layer], downs[layer], gains[layer])
            if not last:
                *sent, pair, gate = call(
                    functools.partial(middle_kernel, half), edges_out + state_out, [scratch] * 3,
                    head_flops + tail_flops, here, *operands, masks[k], projs[layer + 1],
                    gains[layer + 1],
                )
                edges[k] = exchange(sent, width, groups)
                state[k] = (pair, gate)
            else:
                slots = 1 if k else parts
                (done,) = call(
                    functools.partial(last_kernel, half),
                    [((slots, rows, columns, channels), jnp.bfloat16)],
                    [scratch], tail_flops, here, *operands,
                )
                finished[k] = move_parts(done, k, width)
    result = finished[0]
    for k in range(1, parts):
        result = lax.dynamic_update_slice_in_dim(result, finished[k], (part + parts - k) % parts, 0)
    return result


def solution(mesh):
    def step(pair_in, *operands):
        mapped = jax.shard_map(
            per_device,
            mesh=mesh,
            in_specs=(
                P("groups", "axial", None, None),
                P("groups", None),
                P("section", None, None, None),
                P("section", None, None),
                P("section", None, None),
                P("section", None, None),
                P("section", None, None),
            ),
            out_specs=P(("groups", "section"), "axial", None, None),
            check_vma=False,
        )
        return mapped(pair_in, *operands)

    return step
```

```python
import functools

import jax
import jax.numpy as jnp
from jax import lax
from jax.experimental import pallas as pl
from jax.experimental.pallas import tpu as pltpu
from jax.sharding import PartitionSpec as P


epsilon = 1e-05
LANES = 128
TOGETHER = 1024
UNROLL = 32
VMEM_BYTES = 24 * 1024 * 1024


def normalize(values):
    count = values.shape[0]
    center = values - jnp.sum(values, axis=0, keepdims=True) * (1.0 / count)
    spread = jnp.sum(center * center, axis=0, keepdims=True) * (1.0 / count)
    return center * lax.rsqrt(spread + epsilon)


def matmul(a, b):
    return jnp.dot(a, b, preferred_element_type=jnp.float32)


def side_by_side(pieces):
    return pieces[0] if len(pieces) == 1 else jnp.concatenate(pieces, axis=1)


def put_rows(scratch, first, rows, values):
    tiles = scratch.shape[0]
    for place in range(values.shape[1] // LANES):
        scratch[place % tiles, pl.ds(first + place // tiles, values.shape[0], stride=rows), :] = (
            values[:, place * LANES : (place + 1) * LANES]
        )


def take_rows(scratch, first, count, rows, channels):
    return side_by_side(
        [
            scratch[tile, pl.ds(first + row, channels, stride=rows), :]
            for row in range(count)
            for tile in range(scratch.shape[0])
        ]
    )


def read_rows(ref, first, count):
    return side_by_side([ref[first + row] for row in range(count)])


def write_rows(ref, first, values):
    columns = ref.shape[-1]
    for row in range(values.shape[1] // columns):
        ref[first + row] = values[:, row * columns : (row + 1) * columns]


def edges_of_rows(pair_f, row, rows, mask, proj, gain, left_scr, right_scr):
    channels = pair_f.shape[0]
    normed = (normalize(pair_f) * gain).astype(jnp.bfloat16)
    linear = matmul(proj[...], normed)
    p0, p1, p2, p3, p4 = [linear[e * channels : (e + 1) * channels] for e in range(5)]
    put_rows(left_scr, row, rows, (jnp.tanh(p1) + 1.0) * p0 * mask)
    put_rows(right_scr, row, rows, (jnp.tanh(p3) + 1.0) * p2 * mask)
    return 0.5 * jnp.tanh(p4) + 0.5


def write_edges(left_scr, right_scr, here, edges):
    block = edges[0].shape[1]
    for which, scr in enumerate((left_scr, right_scr)):
        for i, edge in enumerate(edges):
            start = pl.multiple_of((here[0] ^ i) * block, block)
            for tile in range(scr.shape[0]):
                edge[which, :, tile * LANES : (tile + 1) * LANES] = scr[
                    tile, pl.ds(start, block), :
                ].astype(jnp.bfloat16)


def repeat(gains, count):
    return side_by_side([gains] * count)


def rows_together(rows, columns):
    return min(rows, max(1, TOGETHER // columns))


def first_kernel(half, here, pair, mask, proj, gains, *refs):
    edges, (pair_t, gate, left_scr, right_scr) = refs[:half], refs[half:]
    rows, columns = pair.shape[:2]
    count = rows_together(rows, columns)

    def step(i, carry):
        row = i * count
        pair_f = side_by_side([pair[row + k].astype(jnp.float32).T for k in range(count)])
        write_rows(pair_t, row, pair_f.astype(jnp.bfloat16))
        opened = edges_of_rows(
            pair_f, row, rows, read_rows(mask, row, count), proj, repeat(gains[0], count),
            left_scr, right_scr,
        )
        write_rows(gate, row, opened.astype(jnp.bfloat16))
        return carry

    lax.fori_loop(0, rows // count, step, 0)
    write_edges(left_scr, right_scr, here, edges)


def triangle_kernel(half, chunks, taken, here, *refs):
    sources = [refs[k * 2 * half : (k + 1) * 2 * half] for k in range(chunks)]
    refs = refs[chunks * 2 * half :]
    products = [refs[n * half : (n + 1) * half] for n in range(len(taken))]
    lefts, rights, sums = refs[len(taken) * half :]
    block, columns = sums.shape[1:]
    places = 2 * half * chunks
    rows = columns // places
    for k in range(chunks):
        for i in range(half):
            chip = lax.rem(here[2] + k, chunks) * half + (here[0] ^ i)
            if k in taken:
                lefts[taken.index(k) * half + i] = sources[k][i][0].astype(jnp.float32)
            rights[2 * chip + here[1]] = sources[k][i][1].astype(jnp.float32)
            rights[2 * chip + 1 - here[1]] = sources[k][half + i][1].astype(jnp.float32)

    def step(c, carry):
        at = pl.ds(pl.multiple_of(c * rows, rows), rows)
        left, right = [
            jnp.concatenate([wide[p, at, :] for p in range(wide.shape[0])], axis=0).astype(
                jnp.bfloat16
            )
            for wide in (lefts, rights)
        ]
        total = lax.dot_general(
            left, right, (((1,), (1,)), ((), ())), preferred_element_type=jnp.float32
        )
        for p in range(half * len(taken)):
            sums[p, at, :] = total[p * rows : (p + 1) * rows]
        return carry

    lax.fori_loop(0, block // rows, step, 0, unroll=min(UNROLL, block // rows))
    for n in range(len(taken)):
        for i in range(half):
            products[n][i][...] = sums[n * half + i].astype(jnp.bfloat16)


def load_product(here, own, prod_scr):
    block = own[0].shape[0]
    for i, piece in enumerate(own):
        values = piece[...].astype(jnp.float32)
        start = pl.multiple_of((here[0] ^ i) * block, block)
        for tile in range(prod_scr.shape[0]):
            prod_scr[tile, pl.ds(start, block), :] = values[:, tile * LANES : (tile + 1) * LANES]


def finish_rows(prod_scr, row, count, pair, gate, out_t, up_t, down_t, gains):
    rows, channels = pair.shape[:2]
    tri = take_rows(prod_scr, row, count, rows, channels)
    tri_norm = (normalize(tri) * repeat(gains[1], count)).astype(jnp.bfloat16)
    opened = read_rows(gate, row, count).astype(jnp.float32)
    mid = read_rows(pair, row, count).astype(jnp.float32) + opened * matmul(out_t[...], tri_norm)
    trans_in = (normalize(mid) * repeat(gains[2], count)).astype(jnp.bfloat16)
    hidden = jnp.maximum(matmul(up_t[...], trans_in), 0.0).astype(jnp.bfloat16)
    return (mid + matmul(down_t[...], hidden)).astype(jnp.bfloat16)


def middle_kernel(half, here, *refs):
    own, refs = refs[:half], refs[half:]
    pair, gate, out_t, up_t, down_t, gains, mask, proj, next_gains = refs[:9]
    edges, refs = refs[9 : 9 + half], refs[9 + half :]
    next_pair, next_gate, prod_scr, left_scr, right_scr = refs
    rows, _, columns = pair.shape
    count = rows_together(rows, columns)
    load_product(here, own, prod_scr)

    def step(i, carry):
        row = i * count
        new = finish_rows(prod_scr, row, count, pair, gate, out_t, up_t, down_t, gains)
        write_rows(next_pair, row, new)
        opened = edges_of_rows(
            new.astype(jnp.float32), row, rows, read_rows(mask, row, count), proj,
            repeat(next_gains[0], count), left_scr, right_scr,
        )
        write_rows(next_gate, row, opened.astype(jnp.bfloat16))
        return carry

    lax.fori_loop(0, rows // count, step, 0)
    write_edges(left_scr, right_scr, here, edges)


def last_kernel(half, here, *refs):
    own, refs = refs[:half], refs[half:]
    pair, gate, out_t, up_t, down_t, gains, result, prod_scr = refs
    rows, _, columns = pair.shape
    count = rows_together(rows, columns)
    slot = here[2] if result.shape[0] > 1 else 0
    load_product(here, own, prod_scr)

    def step(i, carry):
        row = i * count
        new = finish_rows(prod_scr, row, count, pair, gate, out_t, up_t, down_t, gains)
        for k in range(count):
            result[slot, row + k] = (
                new[:, k * columns : (k + 1) * columns].astype(jnp.float32).T.astype(jnp.bfloat16)
            )
        return carry

    lax.fori_loop(0, rows // count, step, 0)


def call(kernel, outs, scratch, flops, here, *operands):
    whole = pl.BlockSpec(memory_space=pltpu.VMEM)
    return pallas(kernel, outs, scratch, flops, whole, here, *operands)


def pallas(kernel, outs, scratch, flops, whole, here, *operands):
    return pl.pallas_call(
        kernel,
        out_shape=[jax.ShapeDtypeStruct(shape, dtype) for shape, dtype in outs],
        in_specs=[pl.BlockSpec(memory_space=pltpu.SMEM)] + [whole] * len(operands),
        out_specs=[whole] * len(outs),
        scratch_shapes=[pltpu.VMEM(shape, jnp.float32) for shape in scratch],
        compiler_params=pltpu.CompilerParams(vmem_limit_bytes=VMEM_BYTES),
        cost_estimate=pl.CostEstimate(flops=flops, bytes_accessed=0, transcendentals=0),
    )(here, *operands)


def exchange(blocks, width, groups):
    half = len(blocks)
    if not by_permutes(width):
        whole = lax.all_to_all(
            jnp.stack(blocks), "axial", 0, 0, tiled=True, axis_index_groups=groups
        )
        return [whole[i] for i in range(half)]
    size = lax.axis_size("axial")
    own = list(blocks)
    for i in range(1, half):
        own[i] = lax.ppermute(blocks[i], "axial", [(j, j ^ (2 * i)) for j in range(size)])
    return own


def with_neighbour(own):
    swap = [(j, j ^ 1) for j in range(lax.axis_size("axial"))]
    if not by_permutes(2 * len(own)):
        whole = lax.ppermute(jnp.stack(own), "axial", swap)
        return own + [whole[i] for i in range(len(own))]
    return own + [lax.ppermute(piece, "axial", swap) for piece in own]


def by_permutes(width):
    return width in (2, 4, 8)


def move_parts(values, distance, width):
    if distance == 0:
        return values
    size = lax.axis_size("axial")
    return lax.ppermute(
        values, "axial", [(j, (j + distance * width) % size) for j in range(size)]
    )


def from_sections(weight, sections):
    return [weight] + [
        lax.ppermute(weight, "section", [((i + shift) % sections, i) for i in range(sections)])
        for shift in range(1, sections)
    ]


def by_layer(slots, section):
    sections = len(slots)
    layers = []
    for layer in range(sections):
        chosen = slots[0]
        for shift in range(1, sections):
            chosen = jnp.where((section + shift) % sections == layer, slots[shift], chosen)
        layers.append(chosen)
    return layers


def per_device(pair_in, crop_mask, proj_weights, out_weights, up_weights, down_weights, norm_gains):
    section = lax.axis_index("section")
    sections = lax.axis_size("section")
    axial = lax.axis_size("axial")
    own_count = pair_in.shape[0] // sections
    rows, columns, channels = pair_in.shape[1:]
    parts = own_count
    width = axial // parts
    half = width // 2
    block = channels // half * rows
    part, place = lax.axis_index("axial") // width, lax.axis_index("axial") % width
    groups = [
        [p * width + 2 * i + core for i in range(half)] for p in range(parts) for core in range(2)
    ]
    chip = place // 2 if by_permutes(width) else 0 * place
    here = jnp.stack((chip, place % 2, part)).astype(jnp.int32)

    pairs = []
    for k in range(parts):
        crop = lax.dynamic_index_in_dim(
            pair_in, section * own_count + (part + parts - k) % parts, 0, keepdims=False
        )
        pairs.append(move_parts(crop, -k, width))
    projs = from_sections(proj_weights[0], sections)
    gains = from_sections(norm_gains[0], sections)
    others = (out_weights[0], up_weights[0], down_weights[0])
    *others, projs[-1] = lax.optimization_barrier((*others, projs[-1]))
    others = [from_sections(w, sections) for w in others]
    projs = [
        (0.5 * w).astype(w.dtype).transpose(0, 2, 1).reshape(-1, channels)
        for w in by_layer(projs, section)
    ]
    outs, ups, downs = [[w.T for w in by_layer(slots, section)] for slots in others]
    gains = [
        jnp.broadcast_to(g.astype(jnp.float32)[:, :, None], g.shape + (columns,))
        for g in by_layer(gains, section)
    ]

    mask_all = lax.dynamic_index_in_dim(
        crop_mask, section * own_count + part, 0, keepdims=False
    ).astype(jnp.float32)
    masks = [
        (
            lax.dynamic_slice_in_dim(
                mask_all, ((part + k) % parts * width + place) * rows, rows
            )[:, None]
            * mask_all
        )[:, None, :]
        for k in range(parts)
    ]

    tiles = columns // LANES
    scratch = (tiles, channels * rows, LANES)
    edges_out = [((2, block, columns), jnp.bfloat16)] * half
    state_out = [
        ((rows, channels, columns), jnp.bfloat16), ((rows, channels, columns), jnp.bfloat16)
    ]
    hidden = ups[0].shape[0]
    points = rows * columns
    head_flops = 2 * points * 5 * channels * channels
    tail_flops = 2 * points * channels * (channels + 2 * hidden)
    edges, state = [None] * parts, [None] * parts
    for k in range(parts):
        *sent, pair, gate = call(
            functools.partial(first_kernel, half), edges_out + state_out, [scratch] * 2,
            head_flops, here, pairs[k], masks[k], projs[0], gains[0],
        )
        edges[k] = exchange(sent, width, groups)
        state[k] = (pair, gate)
    finished = [None] * parts
    for layer in range(sections):
        edges = [with_neighbour(edges[k]) for k in range(parts)]
        last = layer == sections - 1
        order = range(parts - 1, -1, -1) if last else range(parts)
        tri = {}
        for taken in [(k,) for k in order] if last else [tuple(order)]:
            sides = [(n * half, block, columns) for n in (len(taken), 2 * parts, len(taken))]
            products = call(
                functools.partial(triangle_kernel, half, parts, taken),
                [((block, columns), jnp.bfloat16)] * (half * len(taken)), sides,
                2 * channels // width * columns**3 * len(taken) // parts, here, *sum(edges, []),
            )
            for n, k in enumerate(taken):
                tri[k] = exchange(products[n * half : (n + 1) * half], width, groups)
        for k in order:
            operands = (*tri[k], *state[k], outs[layer], ups[layer], downs[layer], gains[layer])
            if not last:
                *sent, pair, gate = call(
                    functools.partial(middle_kernel, half), edges_out + state_out, [scratch] * 3,
                    head_flops + tail_flops, here, *operands, masks[k], projs[layer + 1],
                    gains[layer + 1],
                )
                edges[k] = exchange(sent, width, groups)
                state[k] = (pair, gate)
            else:
                slots = 1 if k else parts
                (done,) = call(
                    functools.partial(last_kernel, half),
                    [((slots, rows, columns, channels), jnp.bfloat16)],
                    [scratch], tail_flops, here, *operands,
                )
                finished[k] = move_parts(done, k, width)
    result = finished[0]
    for k in range(1, parts):
        result = lax.dynamic_update_slice_in_dim(result, finished[k], (part + parts - k) % parts, 0)
    return result


def solution(mesh):
    def step(pair_in, *operands):
        mapped = jax.shard_map(
            per_device,
            mesh=mesh,
            in_specs=(
                P("groups", "axial", None, None),
                P("groups", None),
                P("section", None, None, None),
                P("section", None, None),
                P("section", None, None),
                P("section", None, None),
                P("section", None, None),
            ),
            out_specs=P(("groups", "section"), "axial", None, None),
            check_vma=False,
        )
        return mapped(pair_in, *operands)

    return step
```

```python
import functools

import jax
import jax.numpy as jnp
from jax import lax
from jax.experimental import pallas as pl
from jax.experimental.pallas import tpu as pltpu
from jax.sharding import PartitionSpec as P


epsilon = 1e-05
LANES = 128
TOGETHER = 1024
UNROLL = 32
VMEM_BYTES = 24 * 1024 * 1024


def normalize(values):
    count = values.shape[0]
    center = values - jnp.sum(values, axis=0, keepdims=True) * (1.0 / count)
    spread = jnp.sum(center * center, axis=0, keepdims=True) * (1.0 / count)
    return center * lax.rsqrt(spread + epsilon)


def matmul(a, b):
    return jnp.dot(a, b, preferred_element_type=jnp.float32)


def side_by_side(pieces):
    return pieces[0] if len(pieces) == 1 else jnp.concatenate(pieces, axis=1)


def put_rows(scratch, first, rows, values):
    tiles = scratch.shape[0]
    for place in range(values.shape[1] // LANES):
        scratch[place % tiles, pl.ds(first + place // tiles, values.shape[0], stride=rows), :] = (
            values[:, place * LANES : (place + 1) * LANES]
        )


def take_rows(scratch, first, count, rows, channels):
    return side_by_side(
        [
            scratch[tile, pl.ds(first + row, channels, stride=rows), :]
            for row in range(count)
            for tile in range(scratch.shape[0])
        ]
    )


def read_rows(ref, first, count):
    return side_by_side([ref[first + row] for row in range(count)])


def write_rows(ref, first, values):
    columns = ref.shape[-1]
    for row in range(values.shape[1] // columns):
        ref[first + row] = values[:, row * columns : (row + 1) * columns]


def edges_of_rows(pair_f, row, rows, mask, proj, gain, left_scr, right_scr):
    channels = pair_f.shape[0]
    normed = (normalize(pair_f) * gain).astype(jnp.bfloat16)
    linear = matmul(proj[...], normed)
    p0, p1, p2, p3, p4 = [linear[e * channels : (e + 1) * channels] for e in range(5)]
    put_rows(left_scr, row, rows, (jnp.tanh(p1) + 1.0) * p0 * mask)
    put_rows(right_scr, row, rows, (jnp.tanh(p3) + 1.0) * p2 * mask)
    return 0.5 * jnp.tanh(p4) + 0.5


def write_edges(left_scr, right_scr, here, edges):
    block = edges[0].shape[1]
    for which, scr in enumerate((left_scr, right_scr)):
        for i, edge in enumerate(edges):
            start = pl.multiple_of((here[0] ^ i) * block, block)
            for tile in range(scr.shape[0]):
                edge[which, :, tile * LANES : (tile + 1) * LANES] = scr[
                    tile, pl.ds(start, block), :
                ].astype(jnp.bfloat16)


def repeat(gains, count):
    return side_by_side([gains] * count)


def rows_together(rows, columns):
    return min(rows, max(1, TOGETHER // columns))


def first_kernel(half, here, pair, mask, proj, gains, *refs):
    edges, (pair_t, gate, left_scr, right_scr) = refs[:half], refs[half:]
    rows, columns = pair.shape[:2]
    count = rows_together(rows, columns)

    def step(i, carry):
        row = i * count
        pair_f = side_by_side([pair[row + k].astype(jnp.float32).T for k in range(count)])
        write_rows(pair_t, row, pair_f.astype(jnp.bfloat16))
        opened = edges_of_rows(
            pair_f, row, rows, read_rows(mask, row, count), proj, repeat(gains[0], count),
            left_scr, right_scr,
        )
        write_rows(gate, row, opened.astype(jnp.bfloat16))
        return carry

    lax.fori_loop(0, rows // count, step, 0)
    write_edges(left_scr, right_scr, here, edges)


def triangle_kernel(half, chunks, taken, here, *refs):
    sources = [refs[k * 2 * half : (k + 1) * 2 * half] for k in range(chunks)]
    refs = refs[chunks * 2 * half :]
    products = [refs[n * half : (n + 1) * half] for n in range(len(taken))]
    lefts, rights, sums = refs[len(taken) * half :]
    block, columns = sums.shape[1:]
    places = 2 * half * chunks
    rows = columns // places
    for k in range(chunks):
        for i in range(half):
            chip = lax.rem(here[2] + k, chunks) * half + (here[0] ^ i)
            if k in taken:
                lefts[taken.index(k) * half + i] = sources[k][i][0].astype(jnp.float32)
            rights[2 * chip + here[1]] = sources[k][i][1].astype(jnp.float32)
            rights[2 * chip + 1 - here[1]] = sources[k][half + i][1].astype(jnp.float32)

    def step(c, carry):
        at = pl.ds(pl.multiple_of(c * rows, rows), rows)
        left, right = [
            jnp.concatenate([wide[p, at, :] for p in range(wide.shape[0])], axis=0).astype(
                jnp.bfloat16
            )
            for wide in (lefts, rights)
        ]
        total = lax.dot_general(
            left, right, (((1,), (1,)), ((), ())), preferred_element_type=jnp.float32
        )
        for p in range(half * len(taken)):
            sums[p, at, :] = total[p * rows : (p + 1) * rows]
        return carry

    lax.fori_loop(0, block // rows, step, 0, unroll=min(UNROLL, block // rows))
    for n in range(len(taken)):
        for i in range(half):
            products[n][i][...] = sums[n * half + i].astype(jnp.bfloat16)


def load_product(here, own, prod_scr):
    block = own[0].shape[0]
    for i, piece in enumerate(own):
        values = piece[...].astype(jnp.float32)
        start = pl.multiple_of((here[0] ^ i) * block, block)
        for tile in range(prod_scr.shape[0]):
            prod_scr[tile, pl.ds(start, block), :] = values[:, tile * LANES : (tile + 1) * LANES]


def finish_rows(prod_scr, row, count, pair, gate, out_t, up_t, down_t, gains):
    rows, channels = pair.shape[:2]
    tri = take_rows(prod_scr, row, count, rows, channels)
    tri_norm = (normalize(tri) * repeat(gains[1], count)).astype(jnp.bfloat16)
    opened = read_rows(gate, row, count).astype(jnp.float32)
    mid = read_rows(pair, row, count).astype(jnp.float32) + opened * matmul(out_t[...], tri_norm)
    trans_in = (normalize(mid) * repeat(gains[2], count)).astype(jnp.bfloat16)
    hidden = jnp.maximum(matmul(up_t[...], trans_in), 0.0).astype(jnp.bfloat16)
    return (mid + matmul(down_t[...], hidden)).astype(jnp.bfloat16)


def middle_kernel(half, here, *refs):
    own, refs = refs[:half], refs[half:]
    pair, gate, out_t, up_t, down_t, gains, mask, proj, next_gains = refs[:9]
    edges, refs = refs[9 : 9 + half], refs[9 + half :]
    next_pair, next_gate, prod_scr, left_scr, right_scr = refs
    rows, _, columns = pair.shape
    count = rows_together(rows, columns)
    load_product(here, own, prod_scr)

    def step(i, carry):
        row = i * count
        new = finish_rows(prod_scr, row, count, pair, gate, out_t, up_t, down_t, gains)
        write_rows(next_pair, row, new)
        opened = edges_of_rows(
            new.astype(jnp.float32), row, rows, read_rows(mask, row, count), proj,
            repeat(next_gains[0], count), left_scr, right_scr,
        )
        write_rows(next_gate, row, opened.astype(jnp.bfloat16))
        return carry

    lax.fori_loop(0, rows // count, step, 0)
    write_edges(left_scr, right_scr, here, edges)


def last_kernel(half, here, *refs):
    own, refs = refs[:half], refs[half:]
    pair, gate, out_t, up_t, down_t, gains, result, prod_scr = refs
    rows, _, columns = pair.shape
    count = rows_together(rows, columns)
    slot = here[2] if result.shape[0] > 1 else 0
    load_product(here, own, prod_scr)

    def step(i, carry):
        row = i * count
        new = finish_rows(prod_scr, row, count, pair, gate, out_t, up_t, down_t, gains)
        for k in range(count):
            result[slot, row + k] = (
                new[:, k * columns : (k + 1) * columns].astype(jnp.float32).T.astype(jnp.bfloat16)
            )
        return carry

    lax.fori_loop(0, rows // count, step, 0)


def call(kernel, outs, scratch, flops, here, *operands):
    whole = pl.BlockSpec(memory_space=pltpu.VMEM)
    return pallas(kernel, outs, scratch, flops, whole, here, *operands)


def pallas(kernel, outs, scratch, flops, whole, here, *operands):
    return pl.pallas_call(
        kernel,
        out_shape=[jax.ShapeDtypeStruct(shape, dtype) for shape, dtype in outs],
        in_specs=[pl.BlockSpec(memory_space=pltpu.SMEM)] + [whole] * len(operands),
        out_specs=[whole] * len(outs),
        scratch_shapes=[pltpu.VMEM(shape, jnp.float32) for shape in scratch],
        compiler_params=pltpu.CompilerParams(vmem_limit_bytes=VMEM_BYTES),
        cost_estimate=pl.CostEstimate(flops=flops, bytes_accessed=0, transcendentals=0),
    )(here, *operands)


def exchange(blocks, width, groups):
    half = len(blocks)
    if not by_permutes(width):
        whole = lax.all_to_all(
            jnp.stack(blocks), "axial", 0, 0, tiled=True, axis_index_groups=groups
        )
        return [whole[i] for i in range(half)]
    size = lax.axis_size("axial")
    own = list(blocks)
    for i in range(1, half):
        own[i] = lax.ppermute(blocks[i], "axial", [(j, j ^ (2 * i)) for j in range(size)])
    return own


def with_neighbour(own):
    swap = [(j, j ^ 1) for j in range(lax.axis_size("axial"))]
    if not by_permutes(2 * len(own)):
        whole = lax.ppermute(jnp.stack(own), "axial", swap)
        return own + [whole[i] for i in range(len(own))]
    return own + [lax.ppermute(piece, "axial", swap) for piece in own]


def by_permutes(width):
    return width in (2, 4, 8)


def move_parts(values, distance, width):
    if distance == 0:
        return values
    size = lax.axis_size("axial")
    return lax.ppermute(
        values, "axial", [(j, (j + distance * width) % size) for j in range(size)]
    )


def from_sections(weight, sections):
    return [weight] + [
        lax.ppermute(weight, "section", [((i + shift) % sections, i) for i in range(sections)])
        for shift in range(1, sections)
    ]


def by_layer(slots, section):
    sections = len(slots)
    layers = []
    for layer in range(sections):
        chosen = slots[0]
        for shift in range(1, sections):
            chosen = jnp.where((section + shift) % sections == layer, slots[shift], chosen)
        layers.append(chosen)
    return layers


def per_device(pair_in, crop_mask, proj_weights, out_weights, up_weights, down_weights, norm_gains):
    section = lax.axis_index("section")
    sections = lax.axis_size("section")
    axial = lax.axis_size("axial")
    own_count = pair_in.shape[0] // sections
    rows, columns, channels = pair_in.shape[1:]
    parts = own_count
    width = axial // parts
    half = width // 2
    block = channels // half * rows
    part, place = lax.axis_index("axial") // width, lax.axis_index("axial") % width
    groups = [
        [p * width + 2 * i + core for i in range(half)] for p in range(parts) for core in range(2)
    ]
    chip = place // 2 if by_permutes(width) else 0 * place
    here = jnp.stack((chip, place % 2, part)).astype(jnp.int32)

    pairs = []
    for k in range(parts):
        crop = lax.dynamic_index_in_dim(
            pair_in, section * own_count + (part + parts - k) % parts, 0, keepdims=False
        )
        pairs.append(move_parts(crop, -k, width))
    heads = from_sections(
        jnp.concatenate((proj_weights[0].reshape(-1, channels), norm_gains[0])), sections
    )
    others = from_sections(
        jnp.concatenate((out_weights[0].T, up_weights[0].T, down_weights[0])), sections
    )
    kinds = proj_weights.shape[1]

    def head_of(slots, layer):
        head = by_layer(slots, section)[layer]
        proj = (0.5 * head[: kinds * channels]).astype(head.dtype)
        proj = proj.reshape(kinds, channels, channels).transpose(0, 2, 1).reshape(-1, channels)
        gain = head[kinds * channels :].astype(jnp.float32)[:, :, None]
        return proj, jnp.broadcast_to(gain, (norm_gains.shape[1], channels, columns))

    proj, gain = head_of(heads, 0)
    projs, gains = [proj], [gain]

    mask_all = lax.dynamic_index_in_dim(
        crop_mask, section * own_count + part, 0, keepdims=False
    ).astype(jnp.float32)
    masks = [
        (
            lax.dynamic_slice_in_dim(
                mask_all, ((part + k) % parts * width + place) * rows, rows
            )[:, None]
            * mask_all
        )[:, None, :]
        for k in range(parts)
    ]

    tiles = columns // LANES
    scratch = (tiles, channels * rows, LANES)
    edges_out = [((2, block, columns), jnp.bfloat16)] * half
    state_out = [
        ((rows, channels, columns), jnp.bfloat16), ((rows, channels, columns), jnp.bfloat16)
    ]
    hidden = up_weights.shape[2]
    points = rows * columns
    head_flops = 2 * points * 5 * channels * channels
    tail_flops = 2 * points * channels * (channels + 2 * hidden)
    edges, state = [None] * parts, [None] * parts
    for k in range(parts):
        *sent, pair, gate = call(
            functools.partial(first_kernel, half), edges_out + state_out, [scratch] * 2,
            head_flops, here, pairs[k], masks[k], proj, gain,
        )
        edges[k] = exchange(sent, width, groups)
        state[k] = (pair, gate)
    heads, others, state[-1] = lax.optimization_barrier((heads, others, state[-1]))
    for layer in range(1, sections):
        proj, gain = head_of(heads, layer)
        projs.append(proj)
        gains.append(gain)
    bodies = by_layer(others, section)
    outs = [w[:channels] for w in bodies]
    ups = [w[channels : channels + hidden] for w in bodies]
    downs = [w[channels + hidden :].T for w in bodies]
    finished = [None] * parts
    for layer in range(sections):
        edges = [with_neighbour(edges[k]) for k in range(parts)]
        last = layer == sections - 1
        order = range(parts - 1, -1, -1) if last else range(parts)
        tri = {}
        for taken in [(k,) for k in order] if last else [tuple(order)]:
            sides = [(n * half, block, columns) for n in (len(taken), 2 * parts, len(taken))]
            products = call(
                functools.partial(triangle_kernel, half, parts, taken),
                [((block, columns), jnp.bfloat16)] * (half * len(taken)), sides,
                2 * channels // width * columns**3 * len(taken) // parts, here, *sum(edges, []),
            )
            for n, k in enumerate(taken):
                tri[k] = exchange(products[n * half : (n + 1) * half], width, groups)
        for k in order:
            operands = (*tri[k], *state[k], outs[layer], ups[layer], downs[layer], gains[layer])
            if not last:
                *sent, pair, gate = call(
                    functools.partial(middle_kernel, half), edges_out + state_out, [scratch] * 3,
                    head_flops + tail_flops, here, *operands, masks[k], projs[layer + 1],
                    gains[layer + 1],
                )
                edges[k] = exchange(sent, width, groups)
                state[k] = (pair, gate)
            else:
                slots = 1 if k else parts
                (done,) = call(
                    functools.partial(last_kernel, half),
                    [((slots, rows, columns, channels), jnp.bfloat16)],
                    [scratch], tail_flops, here, *operands,
                )
                finished[k] = move_parts(done, k, width)
    result = finished[0]
    for k in range(1, parts):
        result = lax.dynamic_update_slice_in_dim(result, finished[k], (part + parts - k) % parts, 0)
    return result


def solution(mesh):
    def step(pair_in, *operands):
        mapped = jax.shard_map(
            per_device,
            mesh=mesh,
            in_specs=(
                P("groups", "axial", None, None),
                P("groups", None),
                P("section", None, None, None),
                P("section", None, None),
                P("section", None, None),
                P("section", None, None),
                P("section", None, None),
            ),
            out_specs=P(("groups", "section"), "axial", None, None),
            check_vma=False,
        )
        return mapped(pair_in, *operands)

    return step
```

```python
import functools

import jax
import jax.numpy as jnp
from jax import lax
from jax.experimental import pallas as pl
from jax.experimental.pallas import tpu as pltpu
from jax.sharding import PartitionSpec as P


epsilon = 1e-05
LANES = 128
TOGETHER = 1024
UNROLL = 32
VMEM_BYTES = 24 * 1024 * 1024


def normalize(values):
    count = values.shape[0]
    center = values - jnp.sum(values, axis=0, keepdims=True) * (1.0 / count)
    spread = jnp.sum(center * center, axis=0, keepdims=True) * (1.0 / count)
    return center * lax.rsqrt(spread + epsilon)


def matmul(a, b):
    return jnp.dot(a, b, preferred_element_type=jnp.float32)


def side_by_side(pieces):
    return pieces[0] if len(pieces) == 1 else jnp.concatenate(pieces, axis=1)


def put_rows(scratch, first, rows, values):
    tiles = scratch.shape[0]
    for place in range(values.shape[1] // LANES):
        scratch[place % tiles, pl.ds(first + place // tiles, values.shape[0], stride=rows), :] = (
            values[:, place * LANES : (place + 1) * LANES]
        )


def take_rows(scratch, first, count, rows, channels):
    return side_by_side(
        [
            scratch[tile, pl.ds(first + row, channels, stride=rows), :]
            for row in range(count)
            for tile in range(scratch.shape[0])
        ]
    )


def read_rows(ref, first, count):
    return side_by_side([ref[first + row] for row in range(count)])


def write_rows(ref, first, values):
    columns = ref.shape[-1]
    for row in range(values.shape[1] // columns):
        ref[first + row] = values[:, row * columns : (row + 1) * columns]


def edges_of_rows(pair_f, row, rows, mask, proj, gain, left_scr, right_scr):
    channels = pair_f.shape[0]
    normed = (normalize(pair_f) * gain).astype(jnp.bfloat16)
    linear = matmul(proj[...], normed)
    p0, p1, p2, p3, p4 = [linear[e * channels : (e + 1) * channels] for e in range(5)]
    put_rows(left_scr, row, rows, (jnp.tanh(p1) + 1.0) * p0 * mask)
    put_rows(right_scr, row, rows, (jnp.tanh(p3) + 1.0) * p2 * mask)
    return 0.5 * jnp.tanh(p4) + 0.5


def write_edges(left_scr, right_scr, here, edges):
    block = edges[0].shape[1]
    for which, scr in enumerate((left_scr, right_scr)):
        for i, edge in enumerate(edges):
            start = pl.multiple_of((here[0] ^ i) * block, block)
            for tile in range(scr.shape[0]):
                edge[which, :, tile * LANES : (tile + 1) * LANES] = scr[
                    tile, pl.ds(start, block), :
                ].astype(jnp.bfloat16)


def repeat(gains, count):
    return side_by_side([gains] * count)


def rows_together(rows, columns):
    return min(rows, max(1, TOGETHER // columns))


def first_kernel(half, here, pair, mask, proj, gains, *refs):
    edges, (pair_t, gate, left_scr, right_scr) = refs[:half], refs[half:]
    rows, columns = pair.shape[:2]
    count = rows_together(rows, columns)

    def step(i, carry):
        row = i * count
        pair_f = side_by_side([pair[row + k].astype(jnp.float32).T for k in range(count)])
        write_rows(pair_t, row, pair_f.astype(jnp.bfloat16))
        opened = edges_of_rows(
            pair_f, row, rows, read_rows(mask, row, count), proj, repeat(gains[0], count),
            left_scr, right_scr,
        )
        write_rows(gate, row, opened.astype(jnp.bfloat16))
        return carry

    lax.fori_loop(0, rows // count, step, 0)
    write_edges(left_scr, right_scr, here, edges)


def triangle_kernel(half, chunks, taken, here, *refs):
    sources = [refs[k * 2 * half : (k + 1) * 2 * half] for k in range(chunks)]
    refs = refs[chunks * 2 * half :]
    products = [refs[n * half : (n + 1) * half] for n in range(len(taken))]
    lefts, rights, sums = refs[len(taken) * half :]
    block, columns = sums.shape[1:]
    places = 2 * half * chunks
    rows = columns // places
    for k in range(chunks):
        for i in range(half):
            chip = lax.rem(here[2] + k, chunks) * half + (here[0] ^ i)
            if k in taken:
                lefts[taken.index(k) * half + i] = sources[k][i][0].astype(jnp.float32)
            rights[2 * chip + here[1]] = sources[k][i][1].astype(jnp.float32)
            rights[2 * chip + 1 - here[1]] = sources[k][half + i][1].astype(jnp.float32)

    def step(c, carry):
        at = pl.ds(pl.multiple_of(c * rows, rows), rows)
        left, right = [
            jnp.concatenate([wide[p, at, :] for p in range(wide.shape[0])], axis=0).astype(
                jnp.bfloat16
            )
            for wide in (lefts, rights)
        ]
        total = lax.dot_general(
            left, right, (((1,), (1,)), ((), ())), preferred_element_type=jnp.float32
        )
        for p in range(half * len(taken)):
            sums[p, at, :] = total[p * rows : (p + 1) * rows]
        return carry

    lax.fori_loop(0, block // rows, step, 0, unroll=min(UNROLL, block // rows))
    for n in range(len(taken)):
        for i in range(half):
            products[n][i][...] = sums[n * half + i].astype(jnp.bfloat16)


def load_product(here, own, prod_scr):
    block = own[0].shape[0]
    for i, piece in enumerate(own):
        values = piece[...].astype(jnp.float32)
        start = pl.multiple_of((here[0] ^ i) * block, block)
        for tile in range(prod_scr.shape[0]):
            prod_scr[tile, pl.ds(start, block), :] = values[:, tile * LANES : (tile + 1) * LANES]


def finish_rows(prod_scr, row, count, pair, gate, out_t, up_t, down_t, gains):
    rows, channels = pair.shape[:2]
    tri = take_rows(prod_scr, row, count, rows, channels)
    tri_norm = (normalize(tri) * repeat(gains[1], count)).astype(jnp.bfloat16)
    opened = read_rows(gate, row, count).astype(jnp.float32)
    mid = read_rows(pair, row, count).astype(jnp.float32) + opened * matmul(out_t[...], tri_norm)
    trans_in = (normalize(mid) * repeat(gains[2], count)).astype(jnp.bfloat16)
    hidden = jnp.maximum(matmul(up_t[...], trans_in), 0.0).astype(jnp.bfloat16)
    return (mid + matmul(down_t[...], hidden)).astype(jnp.bfloat16)


def middle_kernel(half, here, *refs):
    own, refs = refs[:half], refs[half:]
    pair, gate, out_t, up_t, down_t, gains, mask, proj, next_gains = refs[:9]
    edges, refs = refs[9 : 9 + half], refs[9 + half :]
    next_pair, next_gate, prod_scr, left_scr, right_scr = refs
    rows, _, columns = pair.shape
    count = rows_together(rows, columns)
    load_product(here, own, prod_scr)

    def step(i, carry):
        row = i * count
        new = finish_rows(prod_scr, row, count, pair, gate, out_t, up_t, down_t, gains)
        write_rows(next_pair, row, new)
        opened = edges_of_rows(
            new.astype(jnp.float32), row, rows, read_rows(mask, row, count), proj,
            repeat(next_gains[0], count), left_scr, right_scr,
        )
        write_rows(next_gate, row, opened.astype(jnp.bfloat16))
        return carry

    lax.fori_loop(0, rows // count, step, 0)
    write_edges(left_scr, right_scr, here, edges)


def last_kernel(half, here, *refs):
    own, refs = refs[:half], refs[half:]
    pair, gate, out_t, up_t, down_t, gains, result, prod_scr = refs
    rows, _, columns = pair.shape
    count = rows_together(rows, columns)
    slot = here[2] if result.shape[0] > 1 else 0
    load_product(here, own, prod_scr)

    def step(i, carry):
        row = i * count
        new = finish_rows(prod_scr, row, count, pair, gate, out_t, up_t, down_t, gains)
        for k in range(count):
            result[slot, row + k] = (
                new[:, k * columns : (k + 1) * columns].astype(jnp.float32).T.astype(jnp.bfloat16)
            )
        return carry

    lax.fori_loop(0, rows // count, step, 0)


def fetch_kernel(index, source, target, arrived):
    copy = pltpu.make_async_copy(source.at[index[0]], target, arrived)
    copy.start()
    copy.wait()


def fetch(source, index):
    return pl.pallas_call(
        fetch_kernel,
        out_shape=jax.ShapeDtypeStruct(source.shape[1:], source.dtype),
        in_specs=[
            pl.BlockSpec(memory_space=pltpu.SMEM), pl.BlockSpec(memory_space=pl.ANY)
        ],
        out_specs=pl.BlockSpec(memory_space=pltpu.VMEM),
        scratch_shapes=[pltpu.SemaphoreType.DMA],
    )(index.astype(jnp.int32).reshape(1), source)


def call(kernel, outs, scratch, flops, here, *operands):
    whole = pl.BlockSpec(memory_space=pltpu.VMEM)
    return pallas(kernel, outs, scratch, flops, whole, here, *operands)


def pallas(kernel, outs, scratch, flops, whole, here, *operands):
    return pl.pallas_call(
        kernel,
        out_shape=[jax.ShapeDtypeStruct(shape, dtype) for shape, dtype in outs],
        in_specs=[pl.BlockSpec(memory_space=pltpu.SMEM)] + [whole] * len(operands),
        out_specs=[whole] * len(outs),
        scratch_shapes=[pltpu.VMEM(shape, jnp.float32) for shape in scratch],
        compiler_params=pltpu.CompilerParams(vmem_limit_bytes=VMEM_BYTES),
        cost_estimate=pl.CostEstimate(flops=flops, bytes_accessed=0, transcendentals=0),
    )(here, *operands)


def exchange(blocks, width, groups):
    half = len(blocks)
    if not by_permutes(width):
        whole = lax.all_to_all(
            jnp.stack(blocks), "axial", 0, 0, tiled=True, axis_index_groups=groups
        )
        return [whole[i] for i in range(half)]
    size = lax.axis_size("axial")
    own = list(blocks)
    for i in range(1, half):
        own[i] = lax.ppermute(blocks[i], "axial", [(j, j ^ (2 * i)) for j in range(size)])
    return own


def with_neighbour(own):
    swap = [(j, j ^ 1) for j in range(lax.axis_size("axial"))]
    if not by_permutes(2 * len(own)):
        whole = lax.ppermute(jnp.stack(own), "axial", swap)
        return own + [whole[i] for i in range(len(own))]
    return own + [lax.ppermute(piece, "axial", swap) for piece in own]


def by_permutes(width):
    return width in (2, 4, 8)


def move_parts(values, distance, width):
    if distance == 0:
        return values
    size = lax.axis_size("axial")
    return lax.ppermute(
        values, "axial", [(j, (j + distance * width) % size) for j in range(size)]
    )


def from_sections(weight, sections):
    return [weight] + [
        lax.ppermute(weight, "section", [((i + shift) % sections, i) for i in range(sections)])
        for shift in range(1, sections)
    ]


def by_layer(slots, section):
    sections = len(slots)
    layers = []
    for layer in range(sections):
        chosen = slots[0]
        for shift in range(1, sections):
            chosen = jnp.where((section + shift) % sections == layer, slots[shift], chosen)
        layers.append(chosen)
    return layers


def per_device(pair_in, crop_mask, proj_weights, out_weights, up_weights, down_weights, norm_gains):
    section = lax.axis_index("section")
    sections = lax.axis_size("section")
    axial = lax.axis_size("axial")
    own_count = pair_in.shape[0] // sections
    rows, columns, channels = pair_in.shape[1:]
    parts = own_count
    width = axial // parts
    half = width // 2
    block = channels // half * rows
    part, place = lax.axis_index("axial") // width, lax.axis_index("axial") % width
    groups = [
        [p * width + 2 * i + core for i in range(half)] for p in range(parts) for core in range(2)
    ]
    chip = place // 2 if by_permutes(width) else 0 * place
    here = jnp.stack((chip, place % 2, part)).astype(jnp.int32)

    pairs = []
    for k in range(parts):
        crop = section * own_count + (part + parts - k) % parts
        if k == 0:
            pairs.append(fetch(pair_in, crop))
            continue
        sent = lax.dynamic_index_in_dim(pair_in, crop, 0, keepdims=False)
        pairs.append(move_parts(sent, -k, width))
    heads = from_sections(
        jnp.concatenate((proj_weights[0].reshape(-1, channels), norm_gains[0])), sections
    )
    others = [from_sections(w[0], sections) for w in (out_weights, up_weights, down_weights)]
    kinds = proj_weights.shape[1]

    def head_of(slots, layer):
        head = by_layer(slots, section)[layer]
        proj = (0.5 * head[: kinds * channels]).astype(head.dtype)
        proj = proj.reshape(kinds, channels, channels).transpose(0, 2, 1).reshape(-1, channels)
        gain = head[kinds * channels :].astype(jnp.float32)[:, :, None]
        return proj, jnp.broadcast_to(gain, (norm_gains.shape[1], channels, columns))

    proj, gain = head_of(heads, 0)
    projs, gains = [proj], [gain]

    mask_all = lax.dynamic_index_in_dim(
        crop_mask, section * own_count + part, 0, keepdims=False
    ).astype(jnp.float32)
    masks = [
        (
            lax.dynamic_slice_in_dim(
                mask_all, ((part + k) % parts * width + place) * rows, rows
            )[:, None]
            * mask_all
        )[:, None, :]
        for k in range(parts)
    ]

    tiles = columns // LANES
    scratch = (tiles, channels * rows, LANES)
    edges_out = [((2, block, columns), jnp.bfloat16)] * half
    state_out = [
        ((rows, channels, columns), jnp.bfloat16), ((rows, channels, columns), jnp.bfloat16)
    ]
    hidden = up_weights.shape[2]
    points = rows * columns
    head_flops = 2 * points * 5 * channels * channels
    tail_flops = 2 * points * channels * (channels + 2 * hidden)
    edges, state = [None] * parts, [None] * parts
    for k in range(parts):
        *sent, pair, gate = call(
            functools.partial(first_kernel, half), edges_out + state_out, [scratch] * 2,
            head_flops, here, pairs[k], masks[k], proj, gain,
        )
        edges[k] = exchange(sent, width, groups)
        state[k] = (pair, gate)
    heads, others, state[-1] = lax.optimization_barrier((heads, others, state[-1]))
    for layer in range(1, sections):
        proj, gain = head_of(heads, layer)
        projs.append(proj)
        gains.append(gain)
    outs, ups, downs = [[w.T for w in by_layer(slots, section)] for slots in others]
    finished = [None] * parts
    for layer in range(sections):
        edges = [with_neighbour(edges[k]) for k in range(parts)]
        last = layer == sections - 1
        order = range(parts - 1, -1, -1) if last else range(parts)
        tri = {}
        for taken in [(k,) for k in order] if last else [tuple(order)]:
            sides = [(n * half, block, columns) for n in (len(taken), 2 * parts, len(taken))]
            products = call(
                functools.partial(triangle_kernel, half, parts, taken),
                [((block, columns), jnp.bfloat16)] * (half * len(taken)), sides,
                2 * channels // width * columns**3 * len(taken) // parts, here, *sum(edges, []),
            )
            for n, k in enumerate(taken):
                tri[k] = exchange(products[n * half : (n + 1) * half], width, groups)
        for k in order:
            operands = (*tri[k], *state[k], outs[layer], ups[layer], downs[layer], gains[layer])
            if not last:
                *sent, pair, gate = call(
                    functools.partial(middle_kernel, half), edges_out + state_out, [scratch] * 3,
                    head_flops + tail_flops, here, *operands, masks[k], projs[layer + 1],
                    gains[layer + 1],
                )
                edges[k] = exchange(sent, width, groups)
                state[k] = (pair, gate)
            else:
                slots = 1 if k else parts
                (done,) = call(
                    functools.partial(last_kernel, half),
                    [((slots, rows, columns, channels), jnp.bfloat16)],
                    [scratch], tail_flops, here, *operands,
                )
                finished[k] = move_parts(done, k, width)
    result = finished[0]
    for k in range(1, parts):
        result = lax.dynamic_update_slice_in_dim(result, finished[k], (part + parts - k) % parts, 0)
    return result


def solution(mesh):
    def step(pair_in, *operands):
        mapped = jax.shard_map(
            per_device,
            mesh=mesh,
            in_specs=(
                P("groups", "axial", None, None),
                P("groups", None),
                P("section", None, None, None),
                P("section", None, None),
                P("section", None, None),
                P("section", None, None),
                P("section", None, None),
            ),
            out_specs=P(("groups", "section"), "axial", None, None),
            check_vma=False,
        )
        return mapped(pair_in, *operands)

    return step
```

```python
import functools

import jax
import jax.numpy as jnp
from jax import lax
from jax.experimental import pallas as pl
from jax.experimental.pallas import tpu as pltpu
from jax.sharding import PartitionSpec as P


epsilon = 1e-05
LANES = 128
TOGETHER = 1024
UNROLL = 32
VMEM_BYTES = 24 * 1024 * 1024


def normalize(values):
    count = values.shape[0]
    center = values - jnp.sum(values, axis=0, keepdims=True) * (1.0 / count)
    spread = jnp.sum(center * center, axis=0, keepdims=True) * (1.0 / count)
    return center * lax.rsqrt(spread + epsilon)


def matmul(a, b):
    return jnp.dot(a, b, preferred_element_type=jnp.float32)


def side_by_side(pieces):
    return pieces[0] if len(pieces) == 1 else jnp.concatenate(pieces, axis=1)


def put_rows(scratch, first, rows, values):
    tiles = scratch.shape[0]
    for place in range(values.shape[1] // LANES):
        scratch[place % tiles, pl.ds(first + place // tiles, values.shape[0], stride=rows), :] = (
            values[:, place * LANES : (place + 1) * LANES]
        )


def take_rows(scratch, first, count, rows, channels):
    return side_by_side(
        [
            scratch[tile, pl.ds(first + row, channels, stride=rows), :]
            for row in range(count)
            for tile in range(scratch.shape[0])
        ]
    )


def read_rows(ref, first, count):
    return side_by_side([ref[first + row] for row in range(count)])


def write_rows(ref, first, values):
    columns = ref.shape[-1]
    for row in range(values.shape[1] // columns):
        ref[first + row] = values[:, row * columns : (row + 1) * columns]


def edges_of_rows(pair_f, row, rows, mask, proj, gain, left_scr, right_scr):
    channels = pair_f.shape[0]
    normed = (normalize(pair_f) * gain).astype(jnp.bfloat16)
    linear = matmul(proj[...], normed)
    p0, p1, p2, p3, p4 = [linear[e * channels : (e + 1) * channels] for e in range(5)]
    put_rows(left_scr, row, rows, (jnp.tanh(p1) + 1.0) * p0 * mask)
    put_rows(right_scr, row, rows, (jnp.tanh(p3) + 1.0) * p2 * mask)
    return 0.5 * jnp.tanh(p4) + 0.5


def write_edges(left_scr, right_scr, here, edges):
    block = edges[0].shape[1]
    for which, scr in enumerate((left_scr, right_scr)):
        for i, edge in enumerate(edges):
            start = pl.multiple_of((here[0] ^ i) * block, block)
            for tile in range(scr.shape[0]):
                edge[which, :, tile * LANES : (tile + 1) * LANES] = scr[
                    tile, pl.ds(start, block), :
                ].astype(jnp.bfloat16)


def repeat(gains, count):
    return side_by_side([gains] * count)


def rows_together(rows, columns):
    return min(rows, max(1, TOGETHER // columns))


def first_kernel(half, here, pair, mask, proj, gains, *refs):
    edges, (pair_t, gate, left_scr, right_scr) = refs[:half], refs[half:]
    rows, columns = pair.shape[:2]
    count = rows_together(rows, columns)

    def step(i, carry):
        row = i * count
        pair_f = side_by_side([pair[row + k].astype(jnp.float32).T for k in range(count)])
        write_rows(pair_t, row, pair_f.astype(jnp.bfloat16))
        opened = edges_of_rows(
            pair_f, row, rows, read_rows(mask, row, count), proj, repeat(gains[0], count),
            left_scr, right_scr,
        )
        write_rows(gate, row, opened.astype(jnp.bfloat16))
        return carry

    lax.fori_loop(0, rows // count, step, 0)
    write_edges(left_scr, right_scr, here, edges)


def triangle_kernel(half, chunks, taken, here, *refs):
    sources = [refs[k * 2 * half : (k + 1) * 2 * half] for k in range(chunks)]
    refs = refs[chunks * 2 * half :]
    products = [refs[n * half : (n + 1) * half] for n in range(len(taken))]
    lefts, rights, sums = refs[len(taken) * half :]
    block, columns = sums.shape[1:]
    places = 2 * half * chunks
    rows = columns // places
    for k in range(chunks):
        for i in range(half):
            chip = lax.rem(here[2] + k, chunks) * half + (here[0] ^ i)
            if k in taken:
                lefts[taken.index(k) * half + i] = sources[k][i][0].astype(jnp.float32)
            rights[2 * chip + here[1]] = sources[k][i][1].astype(jnp.float32)
            rights[2 * chip + 1 - here[1]] = sources[k][half + i][1].astype(jnp.float32)

    def step(c, carry):
        at = pl.ds(pl.multiple_of(c * rows, rows), rows)
        left, right = [
            jnp.concatenate([wide[p, at, :] for p in range(wide.shape[0])], axis=0).astype(
                jnp.bfloat16
            )
            for wide in (lefts, rights)
        ]
        total = lax.dot_general(
            left, right, (((1,), (1,)), ((), ())), preferred_element_type=jnp.float32
        )
        for p in range(half * len(taken)):
            sums[p, at, :] = total[p * rows : (p + 1) * rows]
        return carry

    lax.fori_loop(0, block // rows, step, 0, unroll=min(UNROLL, block // rows))
    for n in range(len(taken)):
        for i in range(half):
            products[n][i][...] = sums[n * half + i].astype(jnp.bfloat16)


def load_product(here, own, prod_scr):
    block = own[0].shape[0]
    for i, piece in enumerate(own):
        values = piece[...].astype(jnp.float32)
        start = pl.multiple_of((here[0] ^ i) * block, block)
        for tile in range(prod_scr.shape[0]):
            prod_scr[tile, pl.ds(start, block), :] = values[:, tile * LANES : (tile + 1) * LANES]


def finish_rows(prod_scr, row, count, pair, gate, out_t, up_t, down_t, gains):
    rows, channels = pair.shape[:2]
    tri = take_rows(prod_scr, row, count, rows, channels)
    tri_norm = (normalize(tri) * repeat(gains[1], count)).astype(jnp.bfloat16)
    opened = read_rows(gate, row, count).astype(jnp.float32)
    mid = read_rows(pair, row, count).astype(jnp.float32) + opened * matmul(out_t[...], tri_norm)
    trans_in = (normalize(mid) * repeat(gains[2], count)).astype(jnp.bfloat16)
    hidden = jnp.maximum(matmul(up_t[...], trans_in), 0.0).astype(jnp.bfloat16)
    return (mid + matmul(down_t[...], hidden)).astype(jnp.bfloat16)


def middle_kernel(half, here, *refs):
    own, refs = refs[:half], refs[half:]
    pair, gate, out_t, up_t, down_t, gains, mask, proj, next_gains = refs[:9]
    edges, refs = refs[9 : 9 + half], refs[9 + half :]
    next_pair, next_gate, prod_scr, left_scr, right_scr = refs
    rows, _, columns = pair.shape
    count = rows_together(rows, columns)
    load_product(here, own, prod_scr)

    def step(i, carry):
        row = i * count
        new = finish_rows(prod_scr, row, count, pair, gate, out_t, up_t, down_t, gains)
        write_rows(next_pair, row, new)
        opened = edges_of_rows(
            new.astype(jnp.float32), row, rows, read_rows(mask, row, count), proj,
            repeat(next_gains[0], count), left_scr, right_scr,
        )
        write_rows(next_gate, row, opened.astype(jnp.bfloat16))
        return carry

    lax.fori_loop(0, rows // count, step, 0)
    write_edges(left_scr, right_scr, here, edges)


def last_kernel(half, here, *refs):
    own, refs = refs[:half], refs[half:]
    pair, gate, out_t, up_t, down_t, gains, result, prod_scr = refs
    rows, _, columns = pair.shape
    count = rows_together(rows, columns)
    slot = here[2] if result.shape[0] > 1 else 0
    load_product(here, own, prod_scr)

    def step(i, carry):
        row = i * count
        new = finish_rows(prod_scr, row, count, pair, gate, out_t, up_t, down_t, gains)
        for k in range(count):
            result[slot, row + k] = (
                new[:, k * columns : (k + 1) * columns].astype(jnp.float32).T.astype(jnp.bfloat16)
            )
        return carry

    lax.fori_loop(0, rows // count, step, 0)


def call(kernel, outs, scratch, flops, here, *operands):
    whole = pl.BlockSpec(memory_space=pltpu.VMEM)
    return pallas(kernel, outs, scratch, flops, whole, here, *operands)


def pallas(kernel, outs, scratch, flops, whole, here, *operands):
    return pl.pallas_call(
        kernel,
        out_shape=[jax.ShapeDtypeStruct(shape, dtype) for shape, dtype in outs],
        in_specs=[pl.BlockSpec(memory_space=pltpu.SMEM)] + [whole] * len(operands),
        out_specs=[whole] * len(outs),
        scratch_shapes=[pltpu.VMEM(shape, jnp.float32) for shape in scratch],
        compiler_params=pltpu.CompilerParams(vmem_limit_bytes=VMEM_BYTES),
        cost_estimate=pl.CostEstimate(flops=flops, bytes_accessed=0, transcendentals=0),
    )(here, *operands)


def exchange(blocks, width, groups):
    half = len(blocks)
    if not by_permutes(width):
        whole = lax.all_to_all(
            jnp.stack(blocks), "axial", 0, 0, tiled=True, axis_index_groups=groups
        )
        return [whole[i] for i in range(half)]
    size = lax.axis_size("axial")
    own = list(blocks)
    for i in range(1, half):
        own[i] = lax.ppermute(blocks[i], "axial", [(j, j ^ (2 * i)) for j in range(size)])
    return own


def with_neighbour(own):
    swap = [(j, j ^ 1) for j in range(lax.axis_size("axial"))]
    if not by_permutes(2 * len(own)):
        whole = lax.ppermute(jnp.stack(own), "axial", swap)
        return own + [whole[i] for i in range(len(own))]
    return own + [lax.ppermute(piece, "axial", swap) for piece in own]


def by_permutes(width):
    return width in (2, 4, 8)


def move_parts(values, distance, width):
    if distance == 0:
        return values
    size = lax.axis_size("axial")
    return lax.ppermute(
        values, "axial", [(j, (j + distance * width) % size) for j in range(size)]
    )


def from_sections(weight, sections):
    return [weight] + [
        lax.ppermute(weight, "section", [((i + shift) % sections, i) for i in range(sections)])
        for shift in range(1, sections)
    ]


def by_layer(slots, section):
    sections = len(slots)
    layers = []
    for layer in range(sections):
        chosen = slots[0]
        for shift in range(1, sections):
            chosen = jnp.where((section + shift) % sections == layer, slots[shift], chosen)
        layers.append(chosen)
    return layers


def per_device(pair_in, crop_mask, proj_weights, out_weights, up_weights, down_weights, norm_gains):
    section = lax.axis_index("section")
    sections = lax.axis_size("section")
    axial = lax.axis_size("axial")
    own_count = pair_in.shape[0] // sections
    rows, columns, channels = pair_in.shape[1:]
    parts = own_count
    width = axial // parts
    half = width // 2
    block = channels // half * rows
    part, place = lax.axis_index("axial") // width, lax.axis_index("axial") % width
    groups = [
        [p * width + 2 * i + core for i in range(half)] for p in range(parts) for core in range(2)
    ]
    chip = place // 2 if by_permutes(width) else 0 * place
    here = jnp.stack((chip, place % 2, part)).astype(jnp.int32)

    pairs = []
    for k in range(parts):
        crop = lax.dynamic_index_in_dim(
            pair_in, section * own_count + (part + parts - k) % parts, 0, keepdims=False
        )
        pairs.append(move_parts(crop, -k, width))
    heads = from_sections(
        jnp.concatenate((proj_weights[0].reshape(-1, channels), norm_gains[0])), sections
    )
    others = [from_sections(w[0], sections) for w in (out_weights, up_weights, down_weights)]
    kinds = proj_weights.shape[1]

    def head_of(slots, layer):
        head = by_layer(slots, section)[layer]
        proj = (0.5 * head[: kinds * channels]).astype(head.dtype)
        proj = proj.reshape(kinds, channels, channels).transpose(0, 2, 1).reshape(-1, channels)
        gain = head[kinds * channels :].astype(jnp.float32)[:, :, None]
        return proj, jnp.broadcast_to(gain, (norm_gains.shape[1], channels, columns))

    proj, gain = head_of(heads, 0)
    projs, gains = [proj], [gain]

    mask_all = lax.dynamic_index_in_dim(
        crop_mask, section * own_count + part, 0, keepdims=False
    ).astype(jnp.float32)
    masks = [
        (
            lax.dynamic_slice_in_dim(
                mask_all, ((part + k) % parts * width + place) * rows, rows
            )[:, None]
            * mask_all
        )[:, None, :]
        for k in range(parts)
    ]

    tiles = columns // LANES
    scratch = (tiles, channels * rows, LANES)
    edges_out = [((2, block, columns), jnp.bfloat16)] * half
    state_out = [
        ((rows, channels, columns), jnp.bfloat16), ((rows, channels, columns), jnp.bfloat16)
    ]
    hidden = up_weights.shape[2]
    points = rows * columns
    head_flops = 2 * points * 5 * channels * channels
    tail_flops = 2 * points * channels * (channels + 2 * hidden)
    edges, state = [None] * parts, [None] * parts
    for k in range(parts):
        *sent, pair, gate = call(
            functools.partial(first_kernel, half), edges_out + state_out, [scratch] * 2,
            head_flops, here, pairs[k], masks[k], proj, gain,
        )
        edges[k] = exchange(sent, width, groups)
        state[k] = (pair, gate)
    heads, others, state[-1] = lax.optimization_barrier((heads, others, state[-1]))
    for layer in range(1, sections):
        proj, gain = head_of(heads, layer)
        projs.append(proj)
        gains.append(gain)
    outs, ups, downs = [[w.T for w in by_layer(slots, section)] for slots in others]
    finished = [None] * parts
    for layer in range(sections):
        edges = [with_neighbour(edges[k]) for k in range(parts)]
        last = layer == sections - 1
        order = range(parts - 1, -1, -1) if last else range(parts)
        tri = {}
        for taken in [tuple(order)]:
            sides = [(n * half, block, columns) for n in (len(taken), 2 * parts, len(taken))]
            products = call(
                functools.partial(triangle_kernel, half, parts, taken),
                [((block, columns), jnp.bfloat16)] * (half * len(taken)), sides,
                2 * channels // width * columns**3 * len(taken) // parts, here, *sum(edges, []),
            )
            for n, k in enumerate(taken):
                tri[k] = exchange(products[n * half : (n + 1) * half], width, groups)
        for k in order:
            operands = (*tri[k], *state[k], outs[layer], ups[layer], downs[layer], gains[layer])
            if not last:
                *sent, pair, gate = call(
                    functools.partial(middle_kernel, half), edges_out + state_out, [scratch] * 3,
                    head_flops + tail_flops, here, *operands, masks[k], projs[layer + 1],
                    gains[layer + 1],
                )
                edges[k] = exchange(sent, width, groups)
                state[k] = (pair, gate)
            else:
                slots = 1 if k else parts
                (done,) = call(
                    functools.partial(last_kernel, half),
                    [((slots, rows, columns, channels), jnp.bfloat16)],
                    [scratch], tail_flops, here, *operands,
                )
                finished[k] = move_parts(done, k, width)
    result = finished[0]
    for k in range(1, parts):
        result = lax.dynamic_update_slice_in_dim(result, finished[k], (part + parts - k) % parts, 0)
    return result


def solution(mesh):
    def step(pair_in, *operands):
        mapped = jax.shard_map(
            per_device,
            mesh=mesh,
            in_specs=(
                P("groups", "axial", None, None),
                P("groups", None),
                P("section", None, None, None),
                P("section", None, None),
                P("section", None, None),
                P("section", None, None),
                P("section", None, None),
            ),
            out_specs=P(("groups", "section"), "axial", None, None),
            check_vma=False,
        )
        return mapped(pair_in, *operands)

    return step
```
